128 devices in a mesh: row: 8 (over z, x_lo), col: 16 (over y, x_hi, core).
Axes of the slice: x: 4 (x_hi: 2, x_lo: 2; x = x_hi * 2 + x_lo), y: 4, z: 4, core: 2. Of those that a mesh axis runs over, the one named last changes fastest.
Arguments:
- cell_index: int32 [2, 3, 262144], P(None, None, ('row', 'col')), may hold values from 0 to 255, as said below
- fraction: float32 [2, 3, 262144], P(None, None, ('row', 'col')), may hold values from 0 to 1
- charge: float32 [2, 262144], P(None, ('row', 'col')), may hold values from -4 to 4
- atom_count: int32 [2, 128], P(None, ('row', 'col')), may hold values from 1024 to 2048, as said below
- influence: float32 [256, 256, 256], P('row', 'col'), as said below
Outputs:
- forces: float32 [2, 3, 262144], P(None, None, ('row', 'col'))
The draws below stay inside these ranges and needn't reach their ends.
Inputs may be any that keep to these rules, and one draw needn't show every extreme that they name: `cell_index`: slot a belongs to pencil p = a // 2048; with P = 16, its first cell index lies in [(p // P) * 32, (p // P + 1) * 32) and its second in [(p % P) * 16, (p % P + 1) * 16). `atom_count`: in every frame some pencil has all 2048 slots live. Even: influence[a, b, c] equals influence[(-a) mod 256, (-b) mod 256, (-c) mod 256]; it is 0 at the root and positive elsewhere.
All inputs are finite; a program needn't handle non-finite values.
Results may differ from the reference program's by a relative error of at most 0.0003.
Values sent between devices are 32-bit elements; how exact they have to be, the bound alone decides.
No kernel may reach another device: no remote copies, remote signals or barrier semaphores. Data moves between devices by JAX's collectives and lax.ppermute only.
A program may use at most 128 MiB of HBM per device.

```python
import math
import jax
import jax.numpy as jnp

K = 256
ATOM_DEV = 2048
STEPS = 2
XB = 32
YB = 16
PENCILS = 128
ATOMS = 262144


def draw_cell_index(key, part):
    per_row = K // YB
    slot_ids = jnp.arange(ATOMS, dtype=jnp.int32)
    pencil = slot_ids // ATOM_DEV
    first_base = pencil // per_row * XB
    second_base = pencil % per_row * YB
    subkeys = jax.random.split(key, 3)
    first_index = first_base[None, :] + jax.random.randint(subkeys[0], (STEPS, ATOMS), 0, XB)
    second_index = second_base[None, :] + jax.random.randint(subkeys[1], (STEPS, ATOMS), 0, YB)
    third_index = jax.random.randint(subkeys[2], (STEPS, ATOMS), 0, K)
    return jnp.stack([first_index, second_index, third_index], axis=1).astype(jnp.int32)


def draw_atom_count(key, part):
    subkeys = jax.random.split(key, 2)
    counts = jax.random.randint(subkeys[0], (STEPS, PENCILS), ATOM_DEV // 2, ATOM_DEV + 1)
    chosen = jax.random.randint(subkeys[1], (STEPS, 1), 0, PENCILS)
    column = jnp.arange(PENCILS, dtype=jnp.int32)
    return jnp.where(column[None, :] == chosen, ATOM_DEV, counts).astype(jnp.int32)


def draw_influence(key, part):
    wave_index = jnp.arange(K, dtype=jnp.int32)
    roughness = jnp.exp(jax.random.uniform(key, (K, K, K), jnp.float32, math.log(2.0), math.log(40.0)))
    mirror = jnp.roll(jnp.flip(roughness, (0, 1, 2)), 1, axis=(0, 1, 2))
    symmetric = 0.5 * (roughness + mirror)
    root = (wave_index[:, None, None] == 0) & (wave_index[None, :, None] == 0) & (wave_index[None, None, :] == 0)
    return jnp.where(root, 0.0, symmetric).astype(jnp.float32)


def steps_of(key, shape, cuts, smallest, high):
    factor_of, own = 1.0, jax.random.fold_in(key, 6)
    for position, blocks in cuts:
        steps = jnp.exp(jax.random.uniform(jax.random.fold_in(own, position), (blocks,), jnp.float32, smallest / len(cuts), high / len(cuts)))
        factor_of = factor_of * jnp.repeat(steps, shape[position] // blocks).reshape([-1 if axis == position else 1 for axis in range(len(shape))])
    return factor_of


def scatter_about(rng, extent, spread, limit, pieces=(), kind=jnp.bfloat16):
    values = jax.random.normal(rng, extent, jnp.float32) * spread
    if len(pieces) > 0:
        values = steps_of(rng, extent, pieces, -0.22, 0.18) * values
    return jnp.clip(values, min=-limit, max=limit).astype(kind)


def setup_inputs(seed: int = 0) -> dict:
    splits = jax.random.split(jax.random.key(seed), 6)
    return {
        "cell_index": draw_cell_index(jax.random.fold_in(splits[5], 71), 0),
        "fraction": jnp.clip(1.0 * jax.random.uniform(splits[1], (STEPS, 3, ATOMS), jnp.float32) ** steps_of(splits[1], (STEPS, 3, ATOMS), ((2, 128),), -0.2, 0.2), 0.0, 1.0),
        "charge": scatter_about(splits[2], (STEPS, ATOMS), 1.0, 4.0, ((1, 128),), jnp.float32),
        "atom_count": draw_atom_count(jax.random.fold_in(splits[5], 71), 0),
        "influence": draw_influence(jax.random.fold_in(splits[5], 71), 0),
    }


def spline_values(fraction):
    nothing = jnp.zeros_like(fraction)
    levels = [fraction, 1.0 - fraction]
    slopes = levels
    for degree in range(3, 7):
        padded = levels + [nothing]
        following = []
        for offset in range(degree):
            beneath = padded[offset - 1] if offset > 0 else nothing
            following.append(((fraction + offset) * padded[offset] + (degree - fraction - offset) * beneath) / (degree - 1))
        if degree == 6:
            slopes = [padded[offset] - (padded[offset - 1] if offset > 0 else nothing) for offset in range(6)]
        levels = following
    return jnp.stack(levels), jnp.stack(slopes)


def reference(cell_index, fraction, charge, atom_count, influence):
    slot_ids = jnp.arange(ATOMS, dtype=jnp.int32)
    pencil = slot_ids // ATOM_DEV
    green_table = jnp.transpose(influence, (2, 0, 1))
    offsets = jnp.arange(6, dtype=jnp.int32)
    results = []
    for step in range(STEPS):
        living = (slot_ids % ATOM_DEV) < atom_count[step][pencil]
        charges = jnp.where(living, charge[step], 0.0)
        values = []
        slopes = []
        corners = []
        for dimension in range(3):
            weight, gradient = spline_values(fraction[step, dimension])
            values.append(weight)
            slopes.append(gradient)
            corners.append(((cell_index[step, dimension][None, :] - offsets[:, None]) % K).astype(jnp.int32))
        index_inner = corners[1][:, None, :] * K + corners[2][None, :, :]
        weight_inner = values[1][:, None, :] * values[2][None, :, :]
        charge_mesh = jnp.zeros((K * K * K,), jnp.float32)
        for offset in range(6):
            target = corners[0][offset][None, None, :] * (K * K) + index_inner
            amount = charges[None, None, :] * values[0][offset][None, None, :] * weight_inner
            charge_mesh = charge_mesh.at[target.reshape(-1)].add(amount.reshape(-1))
        spectrum = jnp.fft.fftn(charge_mesh.reshape(K, K, K))
        potential = jnp.real(jnp.fft.ifftn(green_table * spectrum)).reshape(-1)
        first_total = jnp.zeros_like(charges)
        second_total = jnp.zeros_like(charges)
        third_total = jnp.zeros_like(charges)
        for offset in range(6):
            target = corners[0][offset][None, None, :] * (K * K) + index_inner
            sampled = potential[target]
            first_total = first_total + slopes[0][offset] * jnp.sum(sampled * weight_inner, axis=(0, 1))
            second_total = second_total + values[0][offset] * jnp.sum(sampled * slopes[1][:, None, :] * values[2][None, :, :], axis=(0, 1))
            third_total = third_total + values[0][offset] * jnp.sum(sampled * values[1][:, None, :] * slopes[2][None, :, :], axis=(0, 1))
        results.append(-charges[None, :] * jnp.stack([first_total, second_total, third_total]))
    return jnp.stack(results)
```

```python
import math

import jax
import jax.numpy as jnp
import numpy as np
from jax import lax
from jax.experimental import pallas as pl
from jax.experimental.pallas import tpu as pltpu
from jax.sharding import PartitionSpec as P

F32 = jnp.float32
BF16 = jnp.bfloat16
K = 256
XB = 32
YB = 16
ROWS = 8
COLS = 16
DEV = ROWS * COLS
ATOMS = 2048
CHUNK = 512
RIM = 5
INNER = XB * YB
XRIM = RIM * YB
YRIM = RIM * XB
CRIM = RIM * 8
RIMS = XRIM + YRIM + CRIM
VMEM_ALL = pl.BlockSpec(memory_space=pltpu.VMEM)
SMEM_ALL = pl.BlockSpec(memory_space=pltpu.SMEM)


def halves(values):
    top = values.astype(np.float32).astype(jnp.bfloat16)
    rest = (values - top.astype(np.float64)).astype(np.float32).astype(jnp.bfloat16)
    return top, rest


def z_tables():
    p, d = np.meshgrid(np.arange(2), np.arange(DEV), indexing="ij")
    kz = (16 * (d % COLS) + 2 * (d // COLS) + p).reshape(-1)
    angle = 2.0 * math.pi * ((kz[:, None] * np.arange(K)[None, :]) % K) / K
    return halves(np.cos(angle)) + halves(np.sin(angle))


def x_tables():
    x = np.arange(K)
    angle = 2.0 * math.pi * ((x[:, None] * x[None, :]) % K) / K
    return halves(np.cos(angle)) + halves(np.sin(angle))


def y_table():
    c, low, part, high = np.meshgrid(
        np.arange(COLS), np.arange(4), np.arange(2), np.arange(4), indexing="ij"
    )
    y = (16 * c + 4 * high + low).reshape(-1)
    part = part.reshape(-1)[None, :]
    angle = 2.0 * math.pi * ((np.arange(K)[:, None] * y[None, :]) % K) / K
    cosine, sine = np.cos(angle), np.sin(angle)
    real = np.where(part == 0, cosine, sine)
    imag = np.where(part == 0, -sine, cosine)
    return np.concatenate([real, imag], axis=0)


def split(value):
    top = value.astype(BF16)
    return top, (value - top.astype(F32)).astype(BF16)


def dot(a, b, dims=((1,), (0,))):
    return lax.dot_general(a, b, (dims, ((), ())), preferred_element_type=F32)


def dot3(a, b, dims=((1,), (0,))):
    return dot(a[0], b[0], dims) + dot(a[0], b[1], dims) + dot(a[1], b[0], dims)


def spline_values(fraction):
    nothing = jnp.zeros_like(fraction)
    levels = [fraction, 1.0 - fraction]
    slopes = levels
    for degree in range(3, 7):
        padded = levels + [nothing]
        following = []
        for offset in range(degree):
            beneath = padded[offset - 1] if offset > 0 else nothing
            following.append(
                ((fraction + offset) * padded[offset] + (degree - fraction - offset) * beneath)
                * (1.0 / (degree - 1))
            )
        if degree == 6:
            slopes = [
                padded[offset] - (padded[offset - 1] if offset > 0 else nothing)
                for offset in range(6)
            ]
        levels = following
    return levels, slopes


def placed_rows(cell, values, first, count, wrapped):
    shape = (count, cell.shape[1])
    behind = cell - (lax.broadcasted_iota(jnp.int32, shape, 0) + first)
    if wrapped:
        behind = behind & (K - 1)
    masks = [behind == j for j in range(6)]
    results = []
    for value in values:
        total = jnp.zeros(shape, F32)
        for j in range(6):
            total = jnp.where(masks[j], value[j], total)
        results.append(total)
    return results


def atom_slice(cell_ref, frac_ref, charge_ref, count_ref, s, at):
    lanes = pl.ds(pl.multiple_of(at, CHUNK), CHUNK)
    cells = cell_ref[s, :, lanes]
    levels, slopes = spline_values(frac_ref[s, :, lanes])
    slots = lax.broadcasted_iota(jnp.int32, (1, CHUNK), 1) + at
    charges = jnp.where(slots < count_ref[s, 0], charge_ref[pl.ds(s, 1), lanes], 0.0)

    def dimension(d):
        return [w[d : d + 1] for w in levels], [w[d : d + 1] for w in slopes]

    return cells, dimension, charges


def spread_kernel(count_ref, cell_ref, frac_ref, charge_ref, mesh_ref, xr_ref, yr_ref, cr_ref, ph, pq):
    s, i = pl.program_id(0), pl.program_id(1)
    cells, dimension, charges = atom_slice(cell_ref, frac_ref, charge_ref, count_ref, s, i * CHUNK)
    (first,) = placed_rows(cells[0:1] & (XB - 1), [dimension(0)[0]], -8, XB + 8, False)
    (second,) = placed_rows(cells[1:2] & (YB - 1), [dimension(1)[0]], -8, YB + 8, False)
    (third,) = placed_rows(cells[2:3], [dimension(2)[0]], 0, K, True)
    third = split(third)
    second = second * charges

    def put(at, product):
        top, rest = split(product)
        ph[at : at + product.shape[0], :] = top
        pq[at : at + product.shape[0], :] = rest

    for y in range(YB):
        put(y * XB, second[8 + y : 9 + y] * first[8:])
    for x in range(RIM):
        put(INNER + x * YB, first[3 + x : 4 + x] * second[8:])
    for y in range(RIM):
        put(INNER + XRIM + y * XB, second[3 + y : 4 + y] * first[8:])
    corner = [second[3 + y : 4 + y] * first[:8] for y in range(RIM)] + [jnp.zeros((8, CHUNK), F32)]
    for y in range(0, RIM + 1, 2):
        put(INNER + XRIM + YRIM + y * 8, jnp.concatenate(corner[y : y + 2], axis=0))

    total = dot3((ph[...], pq[...]), third, ((1,), (1,)))
    pieces = (
        (mesh_ref, 0, INNER),
        (xr_ref, INNER, XRIM),
        (yr_ref, INNER + XRIM, YRIM),
        (cr_ref, INNER + XRIM + YRIM, CRIM),
    )

    @pl.when(i == 0)
    def _():
        for ref, at, count in pieces:
            for h in range(2):
                ref[2 * s + h] = total[at : at + count, h * 128 : h * 128 + 128]

    @pl.when(i > 0)
    def _():
        for ref, at, count in pieces:
            for h in range(2):
                ref[2 * s + h] += total[at : at + count, h * 128 : h * 128 + 128]


def forward_z_kernel(mesh_ref, xr_ref, yr_ref, cr_ref, ch, cl, sh, sl, out_ref, m):
    m[...] = mesh_ref[...]
    parts = []
    for s in range(2):
        base = (YB - RIM) * XB
        columns = []
        for h in range(2):
            k = 2 * s + h
            m[k, base : base + YRIM, :] += yr_ref[k]
            for x in range(RIM):
                rows = pl.ds(XB - RIM + x, YB, stride=XB)
                m[k, rows, :] += xr_ref[k, x * YB : x * YB + YB, :]
            for y in range(RIM):
                at = (YB - RIM + y) * XB + XB - 8
                m[k, at : at + 8, :] += cr_ref[k, y * 8 : y * 8 + 8]
            columns.append(m[k].T)
        parts.append(split(jnp.concatenate(columns, axis=0)))
    cosines, sines = (ch[...], cl[...]), (sh[...], sl[...])
    real = dot3(cosines, parts[0]) + dot3(sines, parts[1])
    imag = dot3(cosines, parts[1]) - dot3(sines, parts[0])
    for q, value in enumerate((real, imag)):
        for p in range(2):
            for b in range(4):
                out_ref[pl.ds(p * 8 + q * 4 + b, DEV, stride=16), :] = value[
                    p * DEV : (p + 1) * DEV, b * 128 : (b + 1) * 128
                ]


def exchange_blocks(pieces):
    lane = lax.broadcasted_iota(jnp.int32, pieces[0].shape, 1)
    for bit in (1, 2):
        upper = (lane // 32) & bit == bit
        fresh = list(pieces)
        for v in range(4):
            if v & bit == 0:
                a, b = pieces[v], pieces[v | bit]
                fresh[v] = jnp.where(upper, pltpu.roll(b, 32 * bit, 1), a)
                fresh[v | bit] = jnp.where(upper, b, pltpu.roll(a, 128 - 32 * bit, 1))
        pieces = fresh
    return pieces


def plane_kernel(buf_ref, green_ref, eh, el, th, tl, ch, cl, sh, sl, out_ref, d, o):
    cosines, sines = (ch[...], cl[...]), (sh[...], sl[...])
    for p in range(2):
        for c in range(COLS):
            for g in range(2):
                tiles = []
                for r in range(4):
                    at = ((g * 4 + r) * COLS + c) * 16 + p * 8
                    tiles.append(buf_ref[at : at + 8, :])
                for low, tile in enumerate(exchange_blocks(tiles)):
                    at = (c * 4 + low) * 8
                    d[at : at + 8, g * 128 : g * 128 + 128] = tile
        first = dot3((eh[...], el[...]), split(d[...]))
        real, imag = split(first[:K]), split(first[K:])
        f_real = dot3(real, cosines) + dot3(imag, sines)
        f_imag = dot3(imag, cosines) - dot3(real, sines)
        green = jnp.concatenate(
            [green_ref[(r * 2 + p) * XB : (r * 2 + p + 1) * XB, :] for r in range(ROWS)], axis=0
        ) * (1.0 / float(K) ** 3)
        real, imag = split(f_real * green), split(f_imag * green)
        t_real = split(dot3(real, cosines) - dot3(imag, sines))
        t_imag = split(dot3(imag, cosines) + dot3(real, sines))
        both = tuple(jnp.concatenate([a, b], axis=0) for a, b in zip(t_real, t_imag))
        o[...] = dot3((th[...], tl[...]), both)
        for c in range(COLS):
            for g in range(2):
                tiles = []
                for low in range(4):
                    at = (c * 4 + low) * 8
                    tiles.append(o[at : at + 8, g * 128 : g * 128 + 128])
                for r, tile in enumerate(exchange_blocks(tiles)):
                    at = ((g * 4 + r) * COLS + c) * 16 + p * 8
                    out_ref[at : at + 8, :] = tile


def inverse_z_kernel(buf_ref, ch, cl, sh, sl, field_ref, xr_ref, yr_ref, cr_ref):
    cosines, sines = (ch[...], cl[...]), (sh[...], sl[...])
    parts = []
    for q in range(2):
        columns = []
        for p in range(2):
            blocks = []
            for b in range(4):
                blocks.append(buf_ref[pl.ds(p * 8 + q * 4 + b, DEV, stride=16), :].T)
            columns.append(jnp.concatenate(blocks, axis=0))
        parts.append(split(jnp.concatenate(columns, axis=1)))
    real, imag = parts
    fields = (
        dot3(real, cosines) - dot3(imag, sines),
        dot3(imag, cosines) + dot3(real, sines),
    )
    base = (YB - RIM) * XB
    for k in range(4):
        field_ref[k] = fields[k // 2][:, k % 2 * 128 : k % 2 * 128 + 128]
        yr_ref[k] = field_ref[k, base : base + YRIM, :]
        for x in range(RIM):
            rows = pl.ds(XB - RIM + x, YB, stride=XB)
            xr_ref[k, x * YB : x * YB + YB, :] = field_ref[k, rows, :]
        for y in range(RIM):
            at = (YB - RIM + y) * XB + XB - 8
            cr_ref[k, y * 8 : y * 8 + 8, :] = field_ref[k, at : at + 8, :]


def gather_kernel(count_ref, cell_ref, frac_ref, charge_ref, field_ref, xr_ref, yr_ref, cr_ref, out_ref, fh, fl):
    s, i = pl.program_id(0), pl.program_id(1)

    @pl.when(i == 0)
    def _():
        pieces = (
            (field_ref, 0, INNER),
            (xr_ref, INNER, XRIM),
            (yr_ref, INNER + XRIM, YRIM),
        )
        for h in range(2):
            lanes = slice(h * 128, h * 128 + 128)
            for ref, at, count in pieces:
                top, rest = split(ref[2 * s + h])
                fh[at : at + count, lanes] = top
                fl[at : at + count, lanes] = rest
            at = INNER + XRIM + YRIM
            values = jnp.concatenate([cr_ref[2 * s + h], jnp.zeros((8, 128), F32)], axis=0)
            top, rest = split(values)
            fh[at : at + CRIM + 8, lanes] = top
            fl[at : at + CRIM + 8, lanes] = rest

    at = i * CHUNK
    cells, dimension, charges = atom_slice(cell_ref, frac_ref, charge_ref, count_ref, s, at)
    w1, s1 = placed_rows(cells[0:1] & (XB - 1), dimension(0), -8, XB + 8, False)
    w2, s2 = placed_rows(cells[1:2] & (YB - 1), dimension(1), -8, YB + 8, False)
    w3, s3 = placed_rows(cells[2:3], dimension(2), 0, K, True)
    field = (fh[...], fl[...])
    plain = dot3(field, split(w3))
    sloped = dot3(field, split(s3))

    def gathered(base, size, along, across):
        sums = [jnp.zeros((size, CHUNK), F32) for _ in range(3)]
        for n, (value, slope) in enumerate(along):
            rows = slice(base + n * size, base + (n + 1) * size)
            sums[0] += value * plain[rows]
            sums[1] += slope * plain[rows]
            sums[2] += value * sloped[rows]
        value, slope = across
        return (
            jnp.sum(sums[0] * slope, axis=0, keepdims=True),
            jnp.sum(sums[1] * value, axis=0, keepdims=True),
            jnp.sum(sums[2] * value, axis=0, keepdims=True),
        )

    def row(pair, n):
        return pair[0][n : n + 1], pair[1][n : n + 1]

    xs, ys = (w1, s1), (w2, s2)
    inner = gathered(0, XB, [row(ys, 8 + y) for y in range(YB)], (w1[8:], s1[8:]))
    side = gathered(INNER, YB, [row(xs, 3 + x) for x in range(RIM)], (w2[8:], s2[8:]))
    edge = gathered(INNER + XRIM, XB, [row(ys, 3 + y) for y in range(RIM)], (w1[8:], s1[8:]))
    corner = gathered(INNER + XRIM + YRIM, 8, [row(ys, 3 + y) for y in range(RIM)], (w1[:8], s1[:8]))
    force_x = inner[0] + side[1] + edge[0] + corner[0]
    force_y = inner[1] + side[0] + edge[1] + corner[1]
    force_z = inner[2] + side[2] + edge[2] + corner[2]
    lanes = pl.ds(pl.multiple_of(at, CHUNK), CHUNK)
    out_ref[s, :, lanes] = -charges * jnp.concatenate([force_x, force_y, force_z], axis=0)


def green_kernel(in_ref, out_ref, m):
    for h in range(2):
        lanes = slice(h * 128, h * 128 + 128)
        m[...] = in_ref[:, lanes]
        for k in range(COLS):
            out_ref[k * XB : (k + 1) * XB, lanes] = m[pl.ds(k, XB, stride=COLS), :]


def cost(flops, size):
    return pl.CostEstimate(flops=int(flops), bytes_accessed=int(size), transcendentals=0)


def shape(*dims):
    return jax.ShapeDtypeStruct(dims, F32)


def params(steps=0):
    if steps:
        return pltpu.CompilerParams(dimension_semantics=("arbitrary",) * steps)
    return pltpu.CompilerParams()


def shift(value, rows, cols):
    pairs = []
    for r in range(ROWS):
        for c in range(COLS):
            pairs.append((r * COLS + c, ((r + rows) % ROWS) * COLS + (c + cols) % COLS))
    return lax.ppermute(value, ("row", "col"), pairs)


def everywhere(value):
    return lax.all_to_all(value, ("row", "col"), split_axis=0, concat_axis=0, tiled=True)


def shards(cell_index, fraction, charge, atom_count, influence):
    zc = [jnp.asarray(t) for t in z_tables()]
    xc = [jnp.asarray(t) for t in x_tables()]
    table = y_table()
    ye = [jnp.asarray(t) for t in halves(table)]
    yt = [jnp.asarray(t) for t in halves(np.ascontiguousarray(table.T))]

    green = pl.pallas_call(
        green_kernel,
        out_shape=shape(512, K),
        in_specs=[VMEM_ALL],
        out_specs=VMEM_ALL,
        scratch_shapes=[pltpu.VMEM((512, 128), F32)],
        compiler_params=params(),
        cost_estimate=cost(1e6, 2**20),
        name="green",
    )(influence.reshape(XB * COLS, K))
    green = lax.all_to_all(
        green.reshape(ROWS, 64, K), "row", split_axis=0, concat_axis=0, tiled=True
    ).reshape(512, K)

    atoms_specs = [SMEM_ALL, VMEM_ALL, VMEM_ALL, VMEM_ALL]
    atoms = (atom_count, cell_index, fraction, charge)
    steps = ATOMS // CHUNK
    rim_shapes = [shape(4, XRIM, 128), shape(4, YRIM, 128), shape(4, CRIM, 128)]
    mesh, xr, yr, cr = pl.pallas_call(
        spread_kernel,
        grid=(2, steps),
        out_shape=[shape(4, INNER, 128)] + rim_shapes,
        in_specs=atoms_specs,
        out_specs=[VMEM_ALL] * 4,
        scratch_shapes=[pltpu.VMEM((INNER + RIMS + 8, CHUNK), BF16)] * 2,
        compiler_params=params(2),
        cost_estimate=cost(1.0e10, 2**21),
        name="spread",
    )(*atoms)
    xr, yr, cr = shift(xr, -1, 0), shift(yr, 0, -1), shift(cr, -1, -1)
    packed = pl.pallas_call(
        forward_z_kernel,
        out_shape=shape(DEV * 16, 128),
        in_specs=[VMEM_ALL] * 8,
        out_specs=VMEM_ALL,
        scratch_shapes=[pltpu.VMEM((4, INNER, 128), F32)],
        compiler_params=params(),
        cost_estimate=cost(2.0e9, 2**22),
        name="forward_z",
    )(mesh, xr, yr, cr, *zc)
    packed = everywhere(packed.reshape(DEV, 16, 128)).reshape(DEV * 16, 128)
    packed = pl.pallas_call(
        plane_kernel,
        out_shape=shape(DEV * 16, 128),
        in_specs=[VMEM_ALL] * 10,
        out_specs=VMEM_ALL,
        scratch_shapes=[pltpu.VMEM((512, K), F32)] * 2,
        compiler_params=params(),
        cost_estimate=cost(4.0e9, 2**23),
        name="planes",
    )(packed, green, *ye, *yt, *xc)
    packed = everywhere(packed.reshape(DEV, 16, 128)).reshape(DEV * 16, 128)
    field, xr, yr, cr = pl.pallas_call(
        inverse_z_kernel,
        out_shape=[shape(4, INNER, 128)] + rim_shapes,
        in_specs=[VMEM_ALL] * 5,
        out_specs=[VMEM_ALL] * 4,
        compiler_params=params(),
        cost_estimate=cost(2.0e9, 2**22),
        name="inverse_z",
    )(packed, *zc)
    xr, yr, cr = shift(xr, 1, 0), shift(yr, 0, 1), shift(cr, 1, 1)
    return pl.pallas_call(
        gather_kernel,
        grid=(2, steps),
        out_shape=shape(2, 3, ATOMS),
        in_specs=atoms_specs + [VMEM_ALL] * 4,
        out_specs=VMEM_ALL,
        scratch_shapes=[pltpu.VMEM((INNER + RIMS + 8, K), BF16)] * 2,
        compiler_params=params(2),
        cost_estimate=cost(2.0e10, 2**22),
        name="gather",
    )(*atoms, field, xr, yr, cr)


def solution(mesh):
    placed = (
        P(None, None, ("row", "col")),
        P(None, None, ("row", "col")),
        P(None, ("row", "col")),
        P(None, ("row", "col")),
        P("row", "col", None),
    )
    return jax.shard_map(
        shards, mesh=mesh, in_specs=placed, out_specs=P(None, None, ("row", "col")), check_vma=False
    )
```

```python
import math

import jax
import jax.numpy as jnp
import numpy as np
from jax import lax
from jax.experimental import pallas as pl
from jax.experimental.pallas import tpu as pltpu
from jax.sharding import PartitionSpec as P

F32 = jnp.float32
BF16 = jnp.bfloat16
K = 256
XB = 32
YB = 16
ROWS = 8
COLS = 16
DEV = ROWS * COLS
ATOMS = 2048
CHUNK = 256
RIM = 5
INNER = XB * YB
XRIM = RIM * YB
YRIM = RIM * XB
CRIM = RIM * 8
RIMS = XRIM + YRIM + CRIM
VMEM_ALL = pl.BlockSpec(memory_space=pltpu.VMEM)
SMEM_ALL = pl.BlockSpec(memory_space=pltpu.SMEM)


def halves(values):
    top = values.astype(np.float32).astype(jnp.bfloat16)
    rest = (values - top.astype(np.float64)).astype(np.float32).astype(jnp.bfloat16)
    return top, rest


def z_tables():
    p, d = np.meshgrid(np.arange(2), np.arange(DEV), indexing="ij")
    kz = (16 * (d % COLS) + 2 * (d // COLS) + p).reshape(-1)
    angle = 2.0 * math.pi * ((kz[:, None] * np.arange(K)[None, :]) % K) / K
    return np.stack(halves(np.cos(angle)) + halves(np.sin(angle)))


def x_tables():
    x = np.arange(K)
    angle = 2.0 * math.pi * ((x[:, None] * x[None, :]) % K) / K
    return np.stack(halves(np.cos(angle)) + halves(np.sin(angle)))


def y_table():
    c, low, part, high = np.meshgrid(
        np.arange(COLS), np.arange(4), np.arange(2), np.arange(4), indexing="ij"
    )
    y = (16 * c + 4 * high + low).reshape(-1)
    part = part.reshape(-1)[None, :]
    angle = 2.0 * math.pi * ((np.arange(K)[:, None] * y[None, :]) % K) / K
    cosine, sine = np.cos(angle), np.sin(angle)
    real = np.where(part == 0, cosine, sine)
    imag = np.where(part == 0, -sine, cosine)
    return np.concatenate([real, imag], axis=0)


def split(value):
    top = value.astype(BF16)
    return top, (value - top.astype(F32)).astype(BF16)


def dot(a, b, dims=((1,), (0,))):
    return lax.dot_general(a, b, (dims, ((), ())), preferred_element_type=F32)


def dot3(a, b, dims=((1,), (0,))):
    return dot(a[0], b[0], dims) + dot(a[0], b[1], dims) + dot(a[1], b[0], dims)


def spline_values(fraction):
    nothing = jnp.zeros_like(fraction)
    levels = [fraction, 1.0 - fraction]
    slopes = levels
    for degree in range(3, 7):
        padded = levels + [nothing]
        following = []
        for offset in range(degree):
            beneath = padded[offset - 1] if offset > 0 else nothing
            following.append(
                ((fraction + offset) * padded[offset] + (degree - fraction - offset) * beneath)
                * (1.0 / (degree - 1))
            )
        if degree == 6:
            slopes = [
                padded[offset] - (padded[offset - 1] if offset > 0 else nothing)
                for offset in range(6)
            ]
        levels = following
    return levels, slopes


def placed_rows(cell, values, first, count, wrapped):
    shape = (count, cell.shape[1])
    behind = cell - (lax.broadcasted_iota(jnp.int32, shape, 0) + first)
    if wrapped:
        behind = behind & (K - 1)
    masks = [behind == j for j in range(6)]
    results = []
    for value in values:
        total = jnp.zeros(shape, F32)
        for j in range(6):
            total = jnp.where(masks[j], value[j], total)
        results.append(total)
    return results


def atom_rows(frac_ref, lanes):
    fraction = jnp.concatenate([frac_ref[d, :, lanes] for d in range(3)], axis=0)
    return spline_values(fraction)


def live_charges(charge_ref, count_ref, s, at, lanes):
    slots = lax.broadcasted_iota(jnp.int32, (1, lanes.size), 1) + at
    return jnp.where(slots < count_ref[0, s], charge_ref[s : s + 1, lanes], 0.0)


def pick(rows, d, s):
    return [w[2 * d + s : 2 * d + s + 1] for w in rows]


def plane_rows(cell_ref, tables, s, lanes):
    first = cell_ref[0, s : s + 1, lanes] & (XB - 1)
    second = cell_ref[1, s : s + 1, lanes] & (YB - 1)
    return (
        placed_rows(first, [pick(t, 0, s) for t in tables], -8, XB + 8, False),
        placed_rows(second, [pick(t, 1, s) for t in tables], -8, YB + 8, False),
    )


def put(ph, pq, at, product):
    top, rest = split(product)
    ph[at : at + product.shape[0], :] = top
    pq[at : at + product.shape[0], :] = rest


ALL = pl.ds(0, ATOMS)


def give(total, s, pieces):
    for ref, at, count in pieces:
        for h in range(2):
            ref[2 * s + h] = total[at : at + count, h * 128 : h * 128 + 128]


def spread_rim_kernel(
    count_ref, cell_hbm, frac_hbm, charge_hbm, xr_ref, yr_ref, cr_ref, wh_ref, wl_ref,
    cell_ref, frac_ref, charge_ref, ph, pq, sems,
):
    copies = [
        pltpu.make_async_copy(source, target, sems.at[n])
        for n, (source, target) in enumerate(
            ((cell_hbm, cell_ref), (frac_hbm, frac_ref), (charge_hbm, charge_ref))
        )
    ]
    for copy in copies:
        copy.start()
    for copy in copies:
        copy.wait()
    levels, _ = atom_rows(frac_ref, ALL)
    for s in range(2):
        (first,), (second,) = plane_rows(cell_ref, [levels], s, ALL)
        (third,) = placed_rows(cell_ref[2, s : s + 1, :], [pick(levels, 2, s)], 0, K, True)
        wh_ref[s], wl_ref[s] = split(third)
        second = second * live_charges(charge_ref, count_ref, s, 0, ALL)
        p, q = ph.at[s], pq.at[s]
        for x in range(RIM):
            put(p, q, x * YB, first[3 + x : 4 + x] * second[8:])
        for y in range(RIM):
            put(p, q, XRIM + y * XB, second[3 + y : 4 + y] * first[8:])
        corner = [second[3 + y : 4 + y] * first[:8] for y in range(RIM)]
        corner.append(jnp.zeros((8, ATOMS), F32))
        for y in range(0, RIM + 1, 2):
            put(p, q, XRIM + YRIM + y * 8, jnp.concatenate(corner[y : y + 2], axis=0))
        total = dot3((p[...], q[...]), (wh_ref[s], wl_ref[s]), ((1,), (1,)))
        give(total, s, ((xr_ref, 0, XRIM), (yr_ref, XRIM, YRIM), (cr_ref, XRIM + YRIM, CRIM)))


def spread_kernel(count_ref, cell_ref, frac_ref, charge_ref, wh_ref, wl_ref, mesh_ref, ph, pq):
    levels, _ = atom_rows(frac_ref, ALL)
    for s in range(2):
        (first,), (second,) = plane_rows(cell_ref, [levels], s, ALL)
        second = second * live_charges(charge_ref, count_ref, s, 0, ALL)
        p, q = ph.at[s], pq.at[s]
        for y in range(YB):
            put(p, q, y * XB, second[8 + y : 9 + y] * first[8:])
        total = dot3((p[...], q[...]), (wh_ref[s], wl_ref[s]), ((1,), (1,)))
        give(total, s, ((mesh_ref, 0, INNER),))


def weight_kernel(cell_ref, frac_ref, wh_ref, wl_ref, sh_ref, sl_ref):
    levels, slopes = atom_rows(frac_ref, ALL)
    for s in range(2):
        value, slope = placed_rows(
            cell_ref[2, s : s + 1, :], [pick(levels, 2, s), pick(slopes, 2, s)], 0, K, True
        )
        wh_ref[s], wl_ref[s] = split(value)
        sh_ref[s], sl_ref[s] = split(slope)


def forward_z_kernel(mesh_ref, xr_ref, yr_ref, cr_ref, zc, out_ref, m):
    m[...] = mesh_ref[...]
    parts = []
    for s in range(2):
        base = (YB - RIM) * XB
        columns = []
        for h in range(2):
            k = 2 * s + h
            m[k, base : base + YRIM, :] += yr_ref[k]
            for x in range(RIM):
                rows = pl.ds(XB - RIM + x, YB, stride=XB)
                m[k, rows, :] += xr_ref[k, x * YB : x * YB + YB, :]
            for y in range(RIM):
                at = (YB - RIM + y) * XB + XB - 8
                m[k, at : at + 8, :] += cr_ref[k, y * 8 : y * 8 + 8]
            columns.append(m[k].T)
        parts.append(split(jnp.concatenate(columns, axis=0)))
    cosines, sines = (zc[0], zc[1]), (zc[2], zc[3])
    real = dot3(cosines, parts[0]) + dot3(sines, parts[1])
    imag = dot3(cosines, parts[1]) - dot3(sines, parts[0])
    for q, value in enumerate((real, imag)):
        for p in range(2):
            for b in range(4):
                out_ref[pl.ds(p * 8 + q * 4 + b, DEV, stride=16), :] = value[
                    p * DEV : (p + 1) * DEV, b * 128 : (b + 1) * 128
                ]


def exchange_blocks(pieces):
    lane = lax.broadcasted_iota(jnp.int32, pieces[0].shape, 1)
    for bit in (1, 2):
        upper = (lane // 32) & bit == bit
        fresh = list(pieces)
        for v in range(4):
            if v & bit == 0:
                a, b = pieces[v], pieces[v | bit]
                fresh[v] = jnp.where(upper, pltpu.roll(b, 32 * bit, 1), a)
                fresh[v | bit] = jnp.where(upper, b, pltpu.roll(a, 128 - 32 * bit, 1))
        pieces = fresh
    return pieces


def plane_kernel(buf_ref, green_ref, yc, xc, out_ref, d, o):
    cosines, sines = (xc[0], xc[1]), (xc[2], xc[3])
    for p in range(2):
        for c in range(COLS):
            for g in range(2):
                tiles = []
                for r in range(4):
                    at = ((g * 4 + r) * COLS + c) * 16 + p * 8
                    tiles.append(buf_ref[at : at + 8, :])
                for low, tile in enumerate(exchange_blocks(tiles)):
                    at = (c * 4 + low) * 8
                    d[at : at + 8, g * 128 : g * 128 + 128] = tile
        first = dot3((yc[0], yc[1]), split(d[...]))
        real, imag = split(first[:K]), split(first[K:])
        f_real = dot3(real, cosines) + dot3(imag, sines)
        f_imag = dot3(imag, cosines) - dot3(real, sines)
        green = jnp.concatenate(
            [green_ref[(r * 2 + p) * XB : (r * 2 + p + 1) * XB, :] for r in range(ROWS)], axis=0
        ) * (1.0 / float(K) ** 3)
        real, imag = split(f_real * green), split(f_imag * green)
        t_real = split(dot3(real, cosines) - dot3(imag, sines))
        t_imag = split(dot3(imag, cosines) + dot3(real, sines))
        both = tuple(jnp.concatenate([a, b], axis=0) for a, b in zip(t_real, t_imag))
        o[...] = dot3((yc[2], yc[3]), both)
        for c in range(COLS):
            for g in range(2):
                tiles = []
                for low in range(4):
                    at = (c * 4 + low) * 8
                    tiles.append(o[at : at + 8, g * 128 : g * 128 + 128])
                for r, tile in enumerate(exchange_blocks(tiles)):
                    at = ((g * 4 + r) * COLS + c) * 16 + p * 8
                    out_ref[at : at + 8, :] = tile


def inverse_z_kernel(buf_ref, zc, fh_ref, fl_ref, xr_ref, yr_ref, cr_ref, m):
    cosines, sines = (zc[0], zc[1]), (zc[2], zc[3])
    parts = []
    for q in range(2):
        columns = []
        for p in range(2):
            blocks = []
            for b in range(4):
                blocks.append(buf_ref[pl.ds(p * 8 + q * 4 + b, DEV, stride=16), :].T)
            columns.append(jnp.concatenate(blocks, axis=0))
        parts.append(split(jnp.concatenate(columns, axis=1)))
    real, imag = parts
    fields = (
        dot3(real, cosines) - dot3(imag, sines),
        dot3(imag, cosines) + dot3(real, sines),
    )
    base = (YB - RIM) * XB
    for s in range(2):
        fh_ref[s], fl_ref[s] = split(fields[s])
        for h in range(2):
            k = 2 * s + h
            m[k] = fields[s][:, h * 128 : h * 128 + 128]
            yr_ref[k] = m[k, base : base + YRIM, :]
            for x in range(RIM):
                rows = pl.ds(XB - RIM + x, YB, stride=XB)
                xr_ref[k, x * YB : x * YB + YB, :] = m[k, rows, :]
            for y in range(RIM):
                at = (YB - RIM + y) * XB + XB - 8
                cr_ref[k, y * 8 : y * 8 + 8, :] = m[k, at : at + 8, :]


def row(pair, n):
    return pair[0][n : n + 1], pair[1][n : n + 1]


def weighed(plain, sloped, at, along, across):
    value, slope = across
    size = value.shape[0]
    sums = [None] * 3
    for n, (mine, mine_slope) in enumerate(along):
        rows = slice(at + n * size, at + (n + 1) * size)
        terms = (mine * plain[rows], mine_slope * plain[rows], mine * sloped[rows])
        sums = [term if n == 0 else old + term for old, term in zip(sums, terms)]
    return tuple(
        jnp.sum(total * side, axis=0, keepdims=True)
        for total, side in zip(sums, (slope, value, value))
    )


def chunks(body):
    def step(i, carry):
        at = pl.multiple_of(i * CHUNK, CHUNK)
        body(at, pl.ds(at, CHUNK))
        return carry

    lax.fori_loop(0, ATOMS // CHUNK, step, 0)


def gather_kernel(cell_ref, frac_ref, wh_ref, wl_ref, sh_ref, sl_ref, fh_ref, fl_ref, out_ref):
    def body(at, lanes):
        tables = atom_rows(frac_ref, lanes)
        for s in range(2):
            xs, ys = plane_rows(cell_ref, tables, s, lanes)
            field = fh_ref[s], fl_ref[s]
            plain = dot3(field, (wh_ref[s, :, lanes], wl_ref[s, :, lanes]))
            sloped = dot3(field, (sh_ref[s, :, lanes], sl_ref[s, :, lanes]))
            lines = [row(ys, 8 + y) for y in range(YB)]
            forces = weighed(plain, sloped, 0, lines, (xs[0][8:], xs[1][8:]))
            for d in range(3):
                out_ref[d, s : s + 1, lanes] = forces[d]

    chunks(body)


def gather_rim_kernel(
    count_ref, cell_ref, frac_ref, charge_ref, wh_ref, wl_ref, sh_ref, sl_ref,
    xr_ref, yr_ref, cr_ref, inner_ref, out_ref, fh, fl,
):
    for s in range(2):
        for h in range(2):
            k, columns = 2 * s + h, slice(h * 128, h * 128 + 128)
            corner = jnp.concatenate([cr_ref[k], jnp.zeros((8, 128), F32)], axis=0)
            for value, at in ((xr_ref[k], 0), (yr_ref[k], XRIM), (corner, XRIM + YRIM)):
                top, rest = split(value)
                fh[s, at : at + value.shape[0], columns] = top
                fl[s, at : at + value.shape[0], columns] = rest

    def body(at, lanes):
        tables = atom_rows(frac_ref, lanes)
        for s in range(2):
            xs, ys = plane_rows(cell_ref, tables, s, lanes)
            field = fh[s], fl[s]
            plain = dot3(field, (wh_ref[s, :, lanes], wl_ref[s, :, lanes]))
            sloped = dot3(field, (sh_ref[s, :, lanes], sl_ref[s, :, lanes]))
            lines = [row(ys, 3 + y) for y in range(RIM)]
            columns = [row(xs, 3 + x) for x in range(RIM)]
            side = weighed(plain, sloped, 0, columns, (ys[0][8:], ys[1][8:]))
            edge = weighed(plain, sloped, XRIM, lines, (xs[0][8:], xs[1][8:]))
            corner = weighed(plain, sloped, XRIM + YRIM, lines, (xs[0][:8], xs[1][:8]))
            charges = live_charges(charge_ref, count_ref, s, at, lanes)
            for d, e in ((0, 1), (1, 0), (2, 2)):
                force = inner_ref[d, s : s + 1, lanes] + side[e] + edge[d] + corner[d]
                out_ref[d, s : s + 1, lanes] = -charges * force

    chunks(body)


def green_kernel(in_ref, out_ref, m):
    for h in range(2):
        lanes = slice(h * 128, h * 128 + 128)
        m[...] = in_ref[:, lanes]
        for k in range(COLS):
            out_ref[k * XB : (k + 1) * XB, lanes] = m[pl.ds(k, XB, stride=COLS), :]


def call(kernel, name, flops, out_shape, operands, smem=(), hbm=(), scratch=(), limit=24):
    def spec(n):
        if n in hbm:
            return pl.BlockSpec(memory_space=pltpu.HBM)
        return SMEM_ALL if n in smem else VMEM_ALL

    single = not isinstance(out_shape, list)
    shapes = [out_shape] if single else out_shape
    size = sum(math.prod(v.shape) * v.dtype.itemsize for v in list(operands) + shapes)
    return pl.pallas_call(
        kernel,
        out_shape=out_shape,
        in_specs=[spec(n) for n in range(len(operands))],
        out_specs=VMEM_ALL if single else [VMEM_ALL] * len(shapes),
        scratch_shapes=list(scratch),
        compiler_params=pltpu.CompilerParams(vmem_limit_bytes=limit * 2**20),
        cost_estimate=pl.CostEstimate(flops=int(flops), bytes_accessed=size, transcendentals=0),
        name=name,
    )(*operands)


def shape(*dims, dtype=F32):
    return jax.ShapeDtypeStruct(dims, dtype)


def shift(value, rows, cols):
    pairs = []
    for r in range(ROWS):
        for c in range(COLS):
            pairs.append((r * COLS + c, ((r + rows) % ROWS) * COLS + (c + cols) % COLS))
    return lax.ppermute(value, ("row", "col"), pairs)


def everywhere(value):
    return lax.all_to_all(value, ("row", "col"), split_axis=0, concat_axis=0, tiled=True)


def shards(cell_index, fraction, charge, atom_count, influence):
    zc = jnp.asarray(z_tables())
    xc = jnp.asarray(x_tables())
    table = y_table()
    yc = jnp.asarray(np.stack(halves(table) + halves(np.ascontiguousarray(table.T))))

    cells = jnp.transpose(cell_index, (1, 0, 2))
    fractions = jnp.transpose(fraction, (1, 0, 2))
    counts = jnp.transpose(atom_count, (1, 0))
    atoms = (counts, cells, fractions, charge)
    rim_shapes = [shape(4, XRIM, 128), shape(4, YRIM, 128), shape(4, CRIM, 128)]
    weights = shape(2, K, ATOMS, dtype=BF16)

    xr, yr, cr, wh, wl = call(
        spread_rim_kernel, "spread_rim", 6e9, rim_shapes + [weights] * 2, atoms,
        smem=(0,), hbm=(1, 2, 3),
        scratch=[
            pltpu.VMEM((3, 2, ATOMS), jnp.int32),
            pltpu.VMEM((3, 2, ATOMS), F32),
            pltpu.VMEM((2, ATOMS), F32),
            pltpu.VMEM((2, RIMS + 8, ATOMS), BF16),
            pltpu.VMEM((2, RIMS + 8, ATOMS), BF16),
            pltpu.SemaphoreType.DMA((3,)),
        ],
    )
    xr, yr, cr = shift(xr, -1, 0), shift(yr, 0, -1), shift(cr, -1, -1)
    green = call(
        green_kernel, "green", 1e8, shape(512, K), (influence.reshape(XB * COLS, K),),
        scratch=[pltpu.VMEM((512, 128), F32)],
    )
    green = lax.all_to_all(
        green.reshape(ROWS, 64, K), "row", split_axis=0, concat_axis=0, tiled=True
    ).reshape(512, K)
    mesh = call(
        spread_kernel, "spread", 8e9, shape(4, INNER, 128), atoms + (wh, wl),
        smem=(0,),
        scratch=[pltpu.VMEM((2, INNER, ATOMS), BF16)] * 2,
    )
    packed = call(
        forward_z_kernel, "forward_z", 3e9, shape(DEV * 16, 128), (mesh, xr, yr, cr, zc),
        scratch=[pltpu.VMEM((4, INNER, 128), F32)],
    )
    packed = everywhere(packed.reshape(DEV, 16, 128)).reshape(DEV * 16, 128)
    wh, wl, gh, gl = call(weight_kernel, "weights", 1e10, [weights] * 4, (cells, fractions))
    packed = call(
        plane_kernel, "planes", 6e9, shape(DEV * 16, 128), (packed, green, yc, xc),
        scratch=[pltpu.VMEM((512, K), F32)] * 2,
    )
    packed = everywhere(packed.reshape(DEV, 16, 128)).reshape(DEV * 16, 128)
    fh, fl, xr, yr, cr = call(
        inverse_z_kernel, "inverse_z", 3e9, [shape(2, INNER, K, dtype=BF16)] * 2 + rim_shapes,
        (packed, zc),
        scratch=[pltpu.VMEM((4, INNER, 128), F32)],
    )
    xr, yr, cr = shift(xr, 1, 0), shift(yr, 0, 1), shift(cr, 1, 1)
    inner = call(
        gather_kernel, "gather", 1.2e10, shape(3, 2, ATOMS),
        (cells, fractions, wh, wl, gh, gl, fh, fl),
    )
    forces = call(
        gather_rim_kernel, "gather_rim", 8e9, shape(3, 2, ATOMS),
        atoms + (wh, wl, gh, gl, xr, yr, cr, inner), smem=(0,),
        scratch=[pltpu.VMEM((2, RIMS + 8, K), BF16)] * 2,
    )
    return jnp.transpose(forces, (1, 0, 2))


def solution(mesh):
    placed = (
        P(None, None, ("row", "col")),
        P(None, None, ("row", "col")),
        P(None, ("row", "col")),
        P(None, ("row", "col")),
        P("row", "col", None),
    )
    return jax.shard_map(
        shards, mesh=mesh, in_specs=placed, out_specs=P(None, None, ("row", "col")), check_vma=False
    )
```

```python
import math

import jax
import jax.numpy as jnp
import numpy as np
from jax import lax
from jax.experimental import pallas as pl
from jax.experimental.pallas import tpu as pltpu
from jax.sharding import PartitionSpec as P

F32 = jnp.float32
BF16 = jnp.bfloat16
K = 256
XB = 32
YB = 16
ROWS = 8
COLS = 16
DEV = ROWS * COLS
ATOMS = 2048
CHUNK = 512
RIM = 5
INNER = XB * YB
XRIM = RIM * YB
YRIM = RIM * XB
CRIM = RIM * 8
RIMS = XRIM + YRIM + CRIM
VMEM_ALL = pl.BlockSpec(memory_space=pltpu.VMEM)
SMEM_ALL = pl.BlockSpec(memory_space=pltpu.SMEM)


def halves(values):
    top = values.astype(np.float32).astype(jnp.bfloat16)
    rest = (values - top.astype(np.float64)).astype(np.float32).astype(jnp.bfloat16)
    return top, rest


def z_tables():
    p, d = np.meshgrid(np.arange(2), np.arange(DEV), indexing="ij")
    kz = (16 * (d % COLS) + 2 * (d // COLS) + p).reshape(-1)
    angle = 2.0 * math.pi * ((kz[:, None] * np.arange(K)[None, :]) % K) / K
    return np.stack(halves(np.cos(angle)) + halves(np.sin(angle)))


def x_tables():
    x = np.arange(K)
    angle = 2.0 * math.pi * ((x[:, None] * x[None, :]) % K) / K
    return np.stack(halves(np.cos(angle)) + halves(np.sin(angle)))


def y_table():
    c, low, part, high = np.meshgrid(
        np.arange(COLS), np.arange(4), np.arange(2), np.arange(4), indexing="ij"
    )
    y = (16 * c + 4 * high + low).reshape(-1)
    part = part.reshape(-1)[None, :]
    angle = 2.0 * math.pi * ((np.arange(K)[:, None] * y[None, :]) % K) / K
    cosine, sine = np.cos(angle), np.sin(angle)
    real = np.where(part == 0, cosine, sine)
    imag = np.where(part == 0, -sine, cosine)
    return np.concatenate([real, imag], axis=0)


def split(value):
    top = value.astype(BF16)
    return top, (value - top.astype(F32)).astype(BF16)


def dot(a, b, dims=((1,), (0,))):
    return lax.dot_general(a, b, (dims, ((), ())), preferred_element_type=F32)


def dot3(a, b, dims=((1,), (0,))):
    return dot(a[0], b[0], dims) + dot(a[0], b[1], dims) + dot(a[1], b[0], dims)


def spline_values(fraction):
    nothing = jnp.zeros_like(fraction)
    levels = [fraction, 1.0 - fraction]
    slopes = levels
    for degree in range(3, 7):
        padded = levels + [nothing]
        following = []
        for offset in range(degree):
            beneath = padded[offset - 1] if offset > 0 else nothing
            following.append(
                ((fraction + offset) * padded[offset] + (degree - fraction - offset) * beneath)
                * (1.0 / (degree - 1))
            )
        if degree == 6:
            slopes = [
                padded[offset] - (padded[offset - 1] if offset > 0 else nothing)
                for offset in range(6)
            ]
        levels = following
    return levels, slopes


def placed_rows(cell, values, first, count, wrapped):
    shape = (count, cell.shape[1])
    behind = cell - (lax.broadcasted_iota(jnp.int32, shape, 0) + first)
    if wrapped:
        behind = behind & (K - 1)
    masks = [behind == j for j in range(6)]
    results = []
    for value in values:
        total = jnp.zeros(shape, F32)
        for j in range(6):
            total = jnp.where(masks[j], value[j], total)
        results.append(total)
    return results


def place_tables(cell, values, outs):
    count = cell.shape[1]
    base = (cell - lax.broadcasted_iota(jnp.int32, (16, count), 0)).astype(jnp.int16)
    parts = []
    for value in values:
        rows = [split(jnp.broadcast_to(value[j], (16, count))) for j in range(6)]
        parts.append(([row[0] for row in rows], [row[1] for row in rows]))
    for g in range(K // 16):
        behind = (base - jnp.int16(16 * g)) & jnp.int16(K - 1)
        results = [[jnp.zeros((16, count), BF16)] * 2 for _ in values]
        for j in range(6):
            mask = behind == jnp.int16(j)
            results = [
                [jnp.where(mask, part[n][j], result[n]) for n in range(2)]
                for part, result in zip(parts, results)
            ]
        for result, out in zip(results, outs):
            for n in range(2):
                out[n][g * 16 : g * 16 + 16, :] = result[n]


def atom_rows(frac_ref, lanes):
    fraction = jnp.concatenate([frac_ref[d, :, lanes] for d in range(3)], axis=0)
    return spline_values(fraction)


def live_charges(charge_ref, count_ref, s, at, lanes):
    slots = lax.broadcasted_iota(jnp.int32, (1, lanes.size), 1) + at
    return jnp.where(slots < count_ref[0, s], charge_ref[s : s + 1, lanes], 0.0)


def pick(rows, d, s):
    return [w[2 * d + s : 2 * d + s + 1] for w in rows]


def plane_rows(cell_ref, tables, s, lanes):
    first = cell_ref[0, s : s + 1, lanes] & (XB - 1)
    second = cell_ref[1, s : s + 1, lanes] & (YB - 1)
    return (
        placed_rows(first, [pick(t, 0, s) for t in tables], -8, XB + 8, False),
        placed_rows(second, [pick(t, 1, s) for t in tables], -8, YB + 8, False),
    )


def put(ph, pq, at, product):
    top, rest = split(product)
    ph[at : at + product.shape[0], :] = top
    pq[at : at + product.shape[0], :] = rest


ALL = pl.ds(0, ATOMS)


def give(total, s, pieces):
    for ref, at, count in pieces:
        for h in range(2):
            ref[2 * s + h] = total[at : at + count, h * 128 : h * 128 + 128]


def spread_rim_kernel(
    count_ref, cell_hbm, frac_hbm, charge_hbm, xr_ref, yr_ref, cr_ref,
    cell_ref, frac_ref, charge_ref, ph, pq, wh_ref, wl_ref, sems,
):
    copies = [
        pltpu.make_async_copy(source, target, sems.at[n])
        for n, (source, target) in enumerate(
            ((cell_hbm, cell_ref), (frac_hbm, frac_ref), (charge_hbm, charge_ref))
        )
    ]
    for copy in copies:
        copy.start()
    for copy in copies:
        copy.wait()
    levels, _ = atom_rows(frac_ref, ALL)
    for s in range(2):
        (first,), (second,) = plane_rows(cell_ref, [levels], s, ALL)
        place_tables(cell_ref[2, s : s + 1, :], [pick(levels, 2, s)], [(wh_ref.at[s], wl_ref.at[s])])
        second = second * live_charges(charge_ref, count_ref, s, 0, ALL)
        p, q = ph.at[s], pq.at[s]
        for x in range(RIM):
            put(p, q, x * YB, first[3 + x : 4 + x] * second[8:])
        for y in range(RIM):
            put(p, q, XRIM + y * XB, second[3 + y : 4 + y] * first[8:])
        corner = [second[3 + y : 4 + y] * first[:8] for y in range(RIM)]
        corner.append(jnp.zeros((8, ATOMS), F32))
        for y in range(0, RIM + 1, 2):
            put(p, q, XRIM + YRIM + y * 8, jnp.concatenate(corner[y : y + 2], axis=0))
        total = dot3((p[...], q[...]), (wh_ref[s], wl_ref[s]), ((1,), (1,)))
        give(total, s, ((xr_ref, 0, XRIM), (yr_ref, XRIM, YRIM), (cr_ref, XRIM + YRIM, CRIM)))


def spread_kernel(count_ref, cell_ref, frac_ref, charge_ref, mesh_ref, ph, pq, wh_ref, wl_ref):
    levels, _ = atom_rows(frac_ref, ALL)
    for s in range(2):
        (first,), (second,) = plane_rows(cell_ref, [levels], s, ALL)
        second = second * live_charges(charge_ref, count_ref, s, 0, ALL)
        place_tables(cell_ref[2, s : s + 1, :], [pick(levels, 2, s)], [(wh_ref.at[s], wl_ref.at[s])])
        p, q = ph.at[s], pq.at[s]
        for y in range(YB):
            put(p, q, y * XB, second[8 + y : 9 + y] * first[8:])
        total = dot3((p[...], q[...]), (wh_ref[s], wl_ref[s]), ((1,), (1,)))
        give(total, s, ((mesh_ref, 0, INNER),))


def weight_kernel(cell_ref, frac_ref, wh_ref, wl_ref, sh_ref, sl_ref):
    levels, slopes = atom_rows(frac_ref, ALL)
    for s in range(2):
        place_tables(
            cell_ref[2, s : s + 1, :],
            [pick(levels, 2, s), pick(slopes, 2, s)],
            [(wh_ref.at[s], wl_ref.at[s]), (sh_ref.at[s], sl_ref.at[s])],
        )


def forward_z_kernel(mesh_ref, xr_ref, yr_ref, cr_ref, zc, out_ref, m):
    m[...] = mesh_ref[...]
    parts = []
    for s in range(2):
        base = (YB - RIM) * XB
        columns = []
        for h in range(2):
            k = 2 * s + h
            m[k, base : base + YRIM, :] += yr_ref[k]
            for x in range(RIM):
                rows = pl.ds(XB - RIM + x, YB, stride=XB)
                m[k, rows, :] += xr_ref[k, x * YB : x * YB + YB, :]
            for y in range(RIM):
                at = (YB - RIM + y) * XB + XB - 8
                m[k, at : at + 8, :] += cr_ref[k, y * 8 : y * 8 + 8]
            columns.append(m[k].T)
        parts.append(split(jnp.concatenate(columns, axis=0)))
    cosines, sines = (zc[0], zc[1]), (zc[2], zc[3])
    real = dot3(cosines, parts[0]) + dot3(sines, parts[1])
    imag = dot3(cosines, parts[1]) - dot3(sines, parts[0])
    for q, value in enumerate((real, imag)):
        for p in range(2):
            for b in range(4):
                out_ref[pl.ds(p * 8 + q * 4 + b, DEV, stride=16), :] = value[
                    p * DEV : (p + 1) * DEV, b * 128 : (b + 1) * 128
                ]


def exchange_blocks(pieces):
    lane = lax.broadcasted_iota(jnp.int32, pieces[0].shape, 1)
    for bit in (1, 2):
        upper = (lane // 32) & bit == bit
        fresh = list(pieces)
        for v in range(4):
            if v & bit == 0:
                a, b = pieces[v], pieces[v | bit]
                fresh[v] = jnp.where(upper, pltpu.roll(b, 32 * bit, 1), a)
                fresh[v | bit] = jnp.where(upper, b, pltpu.roll(a, 128 - 32 * bit, 1))
        pieces = fresh
    return pieces


def plane_kernel(buf_ref, green_ref, yc, xc, out_ref, d, o):
    cosines, sines = (xc[0], xc[1]), (xc[2], xc[3])
    planes = range(2)
    for p in planes:
        for c in range(COLS):
            for g in range(2):
                tiles = []
                for r in range(4):
                    at = ((g * 4 + r) * COLS + c) * 16 + p * 8
                    tiles.append(buf_ref[at : at + 8, :])
                for low, tile in enumerate(exchange_blocks(tiles)):
                    at = (c * 4 + low) * 8
                    d[p, at : at + 8, g * 128 : g * 128 + 128] = tile
    first = [dot3((yc[0], yc[1]), split(d[p])) for p in planes]
    parts = [(split(f[:K]), split(f[K:])) for f in first]
    parts = [
        (dot3(real, cosines) + dot3(imag, sines), dot3(imag, cosines) - dot3(real, sines))
        for real, imag in parts
    ]
    scaled = []
    for p in planes:
        green = jnp.concatenate(
            [green_ref[(r * 2 + p) * XB : (r * 2 + p + 1) * XB, :] for r in range(ROWS)], axis=0
        ) * (1.0 / float(K) ** 3)
        scaled.append([split(part * green) for part in parts[p]])
    parts = [
        (
            split(dot3(real, cosines) - dot3(imag, sines)),
            split(dot3(imag, cosines) + dot3(real, sines)),
        )
        for real, imag in scaled
    ]
    for p in planes:
        both = tuple(jnp.concatenate([a, b], axis=0) for a, b in zip(*parts[p]))
        o[p] = dot3((yc[2], yc[3]), both)
    for p in planes:
        for c in range(COLS):
            for g in range(2):
                tiles = []
                for low in range(4):
                    at = (c * 4 + low) * 8
                    tiles.append(o[p, at : at + 8, g * 128 : g * 128 + 128])
                for r, tile in enumerate(exchange_blocks(tiles)):
                    at = ((g * 4 + r) * COLS + c) * 16 + p * 8
                    out_ref[at : at + 8, :] = tile


def inverse_z_kernel(buf_ref, zc, fh_ref, fl_ref, xr_ref, yr_ref, cr_ref, m):
    cosines, sines = (zc[0], zc[1]), (zc[2], zc[3])
    parts = []
    for q in range(2):
        columns = []
        for p in range(2):
            blocks = []
            for b in range(4):
                blocks.append(buf_ref[pl.ds(p * 8 + q * 4 + b, DEV, stride=16), :].T)
            columns.append(jnp.concatenate(blocks, axis=0))
        parts.append(split(jnp.concatenate(columns, axis=1)))
    real, imag = parts
    fields = (
        dot3(real, cosines) - dot3(imag, sines),
        dot3(imag, cosines) + dot3(real, sines),
    )
    base = (YB - RIM) * XB
    for s in range(2):
        fh_ref[s], fl_ref[s] = split(fields[s])
        for h in range(2):
            k = 2 * s + h
            m[k] = fields[s][:, h * 128 : h * 128 + 128]
            yr_ref[k] = m[k, base : base + YRIM, :]
            for x in range(RIM):
                rows = pl.ds(XB - RIM + x, YB, stride=XB)
                xr_ref[k, x * YB : x * YB + YB, :] = m[k, rows, :]
            for y in range(RIM):
                at = (YB - RIM + y) * XB + XB - 8
                cr_ref[k, y * 8 : y * 8 + 8, :] = m[k, at : at + 8, :]


def row(pair, n):
    return pair[0][n : n + 1], pair[1][n : n + 1]


def weighed(plain, sloped, at, along, across):
    value, slope = across
    size = value.shape[0]
    sums = [None] * 3
    for n, (mine, mine_slope) in enumerate(along):
        rows = slice(at + n * size, at + (n + 1) * size)
        terms = (mine * plain[rows], mine_slope * plain[rows], mine * sloped[rows])
        sums = [term if n == 0 else old + term for old, term in zip(sums, terms)]
    return tuple(
        jnp.sum(total * side, axis=0, keepdims=True)
        for total, side in zip(sums, (slope, value, value))
    )


def chunks(body):
    def step(i, carry):
        at = pl.multiple_of(i * CHUNK, CHUNK)
        body(at, pl.ds(at, CHUNK))
        return carry

    lax.fori_loop(0, ATOMS // CHUNK, step, 0)


def gather_kernel(cell_ref, frac_ref, wh_ref, wl_ref, sh_ref, sl_ref, fh_ref, fl_ref, out_ref):
    def body(at, lanes):
        tables = atom_rows(frac_ref, lanes)
        for s in range(2):
            xs, ys = plane_rows(cell_ref, tables, s, lanes)
            field = fh_ref[s], fl_ref[s]
            plain = dot3(field, (wh_ref[s, :, lanes], wl_ref[s, :, lanes]))
            sloped = dot3(field, (sh_ref[s, :, lanes], sl_ref[s, :, lanes]))
            lines = [row(ys, 8 + y) for y in range(YB)]
            forces = weighed(plain, sloped, 0, lines, (xs[0][8:], xs[1][8:]))
            for d in range(3):
                out_ref[d, s : s + 1, lanes] = forces[d]

    chunks(body)


def gather_rim_kernel(
    count_ref, cell_ref, frac_ref, charge_ref, wh_ref, wl_ref, sh_ref, sl_ref,
    xr_ref, yr_ref, cr_ref, inner_ref, out_ref, fh, fl,
):
    for s in range(2):
        for h in range(2):
            k, columns = 2 * s + h, slice(h * 128, h * 128 + 128)
            corner = jnp.concatenate([cr_ref[k], jnp.zeros((8, 128), F32)], axis=0)
            for value, at in ((xr_ref[k], 0), (yr_ref[k], XRIM), (corner, XRIM + YRIM)):
                top, rest = split(value)
                fh[s, at : at + value.shape[0], columns] = top
                fl[s, at : at + value.shape[0], columns] = rest

    def body(at, lanes):
        tables = atom_rows(frac_ref, lanes)
        for s in range(2):
            xs, ys = plane_rows(cell_ref, tables, s, lanes)
            field = fh[s], fl[s]
            plain = dot3(field, (wh_ref[s, :, lanes], wl_ref[s, :, lanes]))
            sloped = dot3(field, (sh_ref[s, :, lanes], sl_ref[s, :, lanes]))
            lines = [row(ys, 3 + y) for y in range(RIM)]
            columns = [row(xs, 3 + x) for x in range(RIM)]
            side = weighed(plain, sloped, 0, columns, (ys[0][8:], ys[1][8:]))
            edge = weighed(plain, sloped, XRIM, lines, (xs[0][8:], xs[1][8:]))
            corner = weighed(plain, sloped, XRIM + YRIM, lines, (xs[0][:8], xs[1][:8]))
            charges = live_charges(charge_ref, count_ref, s, at, lanes)
            for d, e in ((0, 1), (1, 0), (2, 2)):
                force = inner_ref[d, s : s + 1, lanes] + side[e] + edge[d] + corner[d]
                out_ref[d, s : s + 1, lanes] = -charges * force

    chunks(body)


def green_kernel(in_ref, out_ref, m):
    for h in range(2):
        lanes = slice(h * 128, h * 128 + 128)
        m[...] = in_ref[:, lanes]
        for k in range(COLS):
            out_ref[k * XB : (k + 1) * XB, lanes] = m[pl.ds(k, XB, stride=COLS), :]


def call(kernel, name, flops, out_shape, operands, smem=(), hbm=(), scratch=(), limit=24):
    def spec(n):
        if n in hbm:
            return pl.BlockSpec(memory_space=pltpu.HBM)
        return SMEM_ALL if n in smem else VMEM_ALL

    single = not isinstance(out_shape, list)
    shapes = [out_shape] if single else out_shape
    size = sum(math.prod(v.shape) * v.dtype.itemsize for v in list(operands) + shapes)
    return pl.pallas_call(
        kernel,
        out_shape=out_shape,
        in_specs=[spec(n) for n in range(len(operands))],
        out_specs=VMEM_ALL if single else [VMEM_ALL] * len(shapes),
        scratch_shapes=list(scratch),
        compiler_params=pltpu.CompilerParams(vmem_limit_bytes=limit * 2**20),
        cost_estimate=pl.CostEstimate(flops=int(flops), bytes_accessed=size, transcendentals=0),
        name=name,
    )(*operands)


def shape(*dims, dtype=F32):
    return jax.ShapeDtypeStruct(dims, dtype)


def shift(value, rows, cols):
    pairs = []
    for r in range(ROWS):
        for c in range(COLS):
            pairs.append((r * COLS + c, ((r + rows) % ROWS) * COLS + (c + cols) % COLS))
    return lax.ppermute(value, ("row", "col"), pairs)


def everywhere(value):
    return lax.all_to_all(value, ("row", "col"), split_axis=0, concat_axis=0, tiled=True)


def shards(cell_index, fraction, charge, atom_count, influence):
    zc = jnp.asarray(z_tables())
    xc = jnp.asarray(x_tables())
    table = y_table()
    yc = jnp.asarray(np.stack(halves(table) + halves(np.ascontiguousarray(table.T))))

    cells = jnp.transpose(cell_index, (1, 0, 2))
    fractions = jnp.transpose(fraction, (1, 0, 2))
    counts = jnp.transpose(atom_count, (1, 0))
    atoms = (counts, cells, fractions, charge)
    rim_shapes = [shape(4, XRIM, 128), shape(4, YRIM, 128), shape(4, CRIM, 128)]
    weights = shape(2, K, ATOMS, dtype=BF16)

    table = pltpu.VMEM((2, K, ATOMS), BF16)
    xr, yr, cr = call(
        spread_rim_kernel, "spread_rim", 6e9, rim_shapes, atoms,
        smem=(0,), hbm=(1, 2, 3), limit=60,
        scratch=[
            pltpu.VMEM((3, 2, ATOMS), jnp.int32),
            pltpu.VMEM((3, 2, ATOMS), F32),
            pltpu.VMEM((2, ATOMS), F32),
            pltpu.VMEM((2, RIMS + 8, ATOMS), BF16),
            pltpu.VMEM((2, RIMS + 8, ATOMS), BF16),
            table,
            table,
            pltpu.SemaphoreType.DMA((3,)),
        ],
    )
    later, _ = lax.optimization_barrier((influence, cr))
    xr, yr, cr = shift(xr, -1, 0), shift(yr, 0, -1), shift(cr, -1, -1)
    green = call(
        green_kernel, "green", 1e8, shape(512, K), (later.reshape(XB * COLS, K),),
        scratch=[pltpu.VMEM((512, 128), F32)],
    )
    green = lax.all_to_all(
        green.reshape(ROWS, 64, K), "row", split_axis=0, concat_axis=0, tiled=True
    ).reshape(512, K)
    mesh = call(
        spread_kernel, "spread", 8e9, shape(4, INNER, 128), atoms,
        smem=(0,), limit=32,
        scratch=[pltpu.VMEM((2, INNER, ATOMS), BF16)] * 2 + [table] * 2,
    )
    packed = call(
        forward_z_kernel, "forward_z", 3e9, shape(DEV * 16, 128), (mesh, xr, yr, cr, zc),
        scratch=[pltpu.VMEM((4, INNER, 128), F32)],
    )
    packed = everywhere(packed.reshape(DEV, 16, 128)).reshape(DEV * 16, 128)
    wh, wl, gh, gl = call(weight_kernel, "weights", 1e10, [weights] * 4, (cells, fractions))
    packed = call(
        plane_kernel, "planes", 6e9, shape(DEV * 16, 128), (packed, green, yc, xc),
        scratch=[pltpu.VMEM((2, 512, K), F32)] * 2,
    )
    packed = everywhere(packed.reshape(DEV, 16, 128)).reshape(DEV * 16, 128)
    fh, fl, xr, yr, cr = call(
        inverse_z_kernel, "inverse_z", 3e9, [shape(2, INNER, K, dtype=BF16)] * 2 + rim_shapes,
        (packed, zc),
        scratch=[pltpu.VMEM((4, INNER, 128), F32)],
    )
    xr, yr, cr = shift(xr, 1, 0), shift(yr, 0, 1), shift(cr, 1, 1)
    inner = call(
        gather_kernel, "gather", 1.2e10, shape(3, 2, ATOMS),
        (cells, fractions, wh, wl, gh, gl, fh, fl),
    )
    forces = call(
        gather_rim_kernel, "gather_rim", 8e9, shape(3, 2, ATOMS),
        atoms + (wh, wl, gh, gl, xr, yr, cr, inner), smem=(0,),
        scratch=[pltpu.VMEM((2, RIMS + 8, K), BF16)] * 2,
    )
    return jnp.transpose(forces, (1, 0, 2))


def solution(mesh):
    placed = (
        P(None, None, ("row", "col")),
        P(None, None, ("row", "col")),
        P(None, ("row", "col")),
        P(None, ("row", "col")),
        P("row", "col", None),
    )
    return jax.shard_map(
        shards, mesh=mesh, in_specs=placed, out_specs=P(None, None, ("row", "col")), check_vma=False
    )
```

```python
import math

import jax
import jax.numpy as jnp
import numpy as np
from jax import lax
from jax.experimental import pallas as pl
from jax.experimental.pallas import tpu as pltpu
from jax.sharding import PartitionSpec as P

F32 = jnp.float32
BF16 = jnp.bfloat16
K = 256
XB = 32
YB = 16
ROWS = 8
COLS = 16
DEV = ROWS * COLS
ATOMS = 2048
CHUNK = 512
RIM = 5
INNER = XB * YB
XRIM = RIM * YB
YRIM = RIM * XB
CRIM = RIM * 8
RIMS = XRIM + YRIM + CRIM
VMEM_ALL = pl.BlockSpec(memory_space=pltpu.VMEM)
HBM_ALL = pl.BlockSpec(memory_space=pltpu.HBM)
SMEM_ALL = pl.BlockSpec(memory_space=pltpu.SMEM)


def halves(values):
    top = values.astype(np.float32).astype(jnp.bfloat16)
    rest = (values - top.astype(np.float64)).astype(np.float32).astype(jnp.bfloat16)
    return top, rest


def z_tables():
    p, d = np.meshgrid(np.arange(2), np.arange(DEV), indexing="ij")
    kz = (16 * (d % COLS) + 2 * (d // COLS) + p).reshape(-1)
    angle = 2.0 * math.pi * ((kz[:, None] * np.arange(K)[None, :]) % K) / K
    return np.stack(halves(np.cos(angle)) + halves(np.sin(angle)))


def x_tables():
    x = np.arange(K)
    angle = 2.0 * math.pi * ((x[:, None] * x[None, :]) % K) / K
    return np.stack(halves(np.cos(angle)) + halves(np.sin(angle)))


def y_table():
    c, low, part, high = np.meshgrid(
        np.arange(COLS), np.arange(4), np.arange(2), np.arange(4), indexing="ij"
    )
    y = (16 * c + 4 * high + low).reshape(-1)
    part = part.reshape(-1)[None, :]
    angle = 2.0 * math.pi * ((np.arange(K)[:, None] * y[None, :]) % K) / K
    cosine, sine = np.cos(angle), np.sin(angle)
    real = np.where(part == 0, cosine, sine)
    imag = np.where(part == 0, -sine, cosine)
    return np.concatenate([real, imag], axis=0)


def split(value):
    top = value.astype(BF16)
    return top, (value - top.astype(F32)).astype(BF16)


def dot(a, b, dims=((1,), (0,))):
    return lax.dot_general(a, b, (dims, ((), ())), preferred_element_type=F32)


def dot3(a, b, dims=((1,), (0,))):
    return dot(a[0], b[0], dims) + dot(a[0], b[1], dims) + dot(a[1], b[0], dims)


def spline_values(fraction):
    nothing = jnp.zeros_like(fraction)
    levels = [fraction, 1.0 - fraction]
    slopes = levels
    for degree in range(3, 7):
        padded = levels + [nothing]
        following = []
        for offset in range(degree):
            beneath = padded[offset - 1] if offset > 0 else nothing
            following.append(
                ((fraction + offset) * padded[offset] + (degree - fraction - offset) * beneath)
                * (1.0 / (degree - 1))
            )
        if degree == 6:
            slopes = [
                padded[offset] - (padded[offset - 1] if offset > 0 else nothing)
                for offset in range(6)
            ]
        levels = following
    return levels, slopes


def placed_rows(cell, values, first, count, wrapped):
    shape = (count, cell.shape[1])
    behind = cell - (lax.broadcasted_iota(jnp.int32, shape, 0) + first)
    if wrapped:
        behind = behind & (K - 1)
    masks = [behind == j for j in range(6)]
    results = []
    for value in values:
        total = jnp.zeros(shape, F32)
        for j in range(6):
            total = jnp.where(masks[j], value[j], total)
        results.append(total)
    return results


def place_tables(cell, values, outs):
    count = cell.shape[1]
    base = (cell - lax.broadcasted_iota(jnp.int32, (16, count), 0)).astype(jnp.int16)
    parts = []
    for value in values:
        rows = [split(jnp.broadcast_to(value[j], (16, count))) for j in range(6)]
        parts.append(([row[0] for row in rows], [row[1] for row in rows]))
    for g in range(K // 16):
        behind = (base - jnp.int16(16 * g)) & jnp.int16(K - 1)
        results = [[jnp.zeros((16, count), BF16)] * 2 for _ in values]
        for j in range(6):
            mask = behind == jnp.int16(j)
            results = [
                [jnp.where(mask, part[n][j], result[n]) for n in range(2)]
                for part, result in zip(parts, results)
            ]
        for result, out in zip(results, outs):
            for n in range(2):
                out[n][g * 16 : g * 16 + 16, :] = result[n]


def atom_rows(frac_ref, lanes):
    fraction = jnp.concatenate([frac_ref[d, :, lanes] for d in range(3)], axis=0)
    return spline_values(fraction)


def live_charges(charge_ref, count_ref, s, at, lanes):
    slots = lax.broadcasted_iota(jnp.int32, (1, lanes.size), 1) + at
    return jnp.where(slots < count_ref[0, s], charge_ref[s : s + 1, lanes], 0.0)


def pick(rows, d, s):
    return [w[2 * d + s : 2 * d + s + 1] for w in rows]


def plane_rows(cell_ref, tables, s, lanes):
    first = cell_ref[0, s : s + 1, lanes] & (XB - 1)
    second = cell_ref[1, s : s + 1, lanes] & (YB - 1)
    return (
        placed_rows(first, [pick(t, 0, s) for t in tables], -8, XB + 8, False),
        placed_rows(second, [pick(t, 1, s) for t in tables], -8, YB + 8, False),
    )


def put(ph, pq, at, product):
    top, rest = split(product)
    ph[at : at + product.shape[0], :] = top
    pq[at : at + product.shape[0], :] = rest


ALL = pl.ds(0, ATOMS)


def give(total, s, pieces):
    for ref, at, count in pieces:
        for h in range(2):
            ref[2 * s + h] = total[at : at + count, h * 128 : h * 128 + 128]


def spread_rim_kernel(
    count_ref, cell_hbm, frac_hbm, charge_hbm, xr_ref, yr_ref, cr_ref,
    cell_ref, frac_ref, charge_ref, ph, pq, wh_ref, wl_ref, sems,
):
    copies = [
        pltpu.make_async_copy(source, target, sems.at[n])
        for n, (source, target) in enumerate(
            ((cell_hbm, cell_ref), (frac_hbm, frac_ref), (charge_hbm, charge_ref))
        )
    ]
    for copy in copies:
        copy.start()
    for copy in copies:
        copy.wait()
    levels, _ = atom_rows(frac_ref, ALL)
    for s in range(2):
        (first,), (second,) = plane_rows(cell_ref, [levels], s, ALL)
        place_tables(cell_ref[2, s : s + 1, :], [pick(levels, 2, s)], [(wh_ref.at[s], wl_ref.at[s])])
        second = second * live_charges(charge_ref, count_ref, s, 0, ALL)
        p, q = ph.at[s], pq.at[s]
        for x in range(RIM):
            put(p, q, x * YB, first[3 + x : 4 + x] * second[8:])
        for y in range(RIM):
            put(p, q, XRIM + y * XB, second[3 + y : 4 + y] * first[8:])
        corner = [second[3 + y : 4 + y] * first[:8] for y in range(RIM)]
        corner.append(jnp.zeros((8, ATOMS), F32))
        for y in range(0, RIM + 1, 2):
            put(p, q, XRIM + YRIM + y * 8, jnp.concatenate(corner[y : y + 2], axis=0))
        total = dot3((p[...], q[...]), (wh_ref[s], wl_ref[s]), ((1,), (1,)))
        give(total, s, ((xr_ref, 0, XRIM), (yr_ref, XRIM, YRIM), (cr_ref, XRIM + YRIM, CRIM)))


def spread_kernel(count_ref, cell_ref, frac_ref, charge_ref, mesh_ref, ph, pq, wh_ref, wl_ref):
    levels, _ = atom_rows(frac_ref, ALL)
    for s in range(2):
        (first,), (second,) = plane_rows(cell_ref, [levels], s, ALL)
        second = second * live_charges(charge_ref, count_ref, s, 0, ALL)
        place_tables(cell_ref[2, s : s + 1, :], [pick(levels, 2, s)], [(wh_ref.at[s], wl_ref.at[s])])
        p, q = ph.at[s], pq.at[s]
        for y in range(YB):
            put(p, q, y * XB, second[8 + y : 9 + y] * first[8:])
        total = dot3((p[...], q[...]), (wh_ref[s], wl_ref[s]), ((1,), (1,)))
        give(total, s, ((mesh_ref, 0, INNER),))


TALL, WIDE = XB + 8, YB + 8
SIDES = 2 * TALL + 2 * WIDE


def weight_kernel(count_ref, cell_ref, frac_ref, charge_ref, wh_ref, wl_ref, sh_ref, sl_ref, xy_ref):
    tables = atom_rows(frac_ref, ALL)
    for s in range(2):
        place_tables(
            cell_ref[2, s : s + 1, :],
            [pick(t, 2, s) for t in tables],
            [(wh_ref.at[s], wl_ref.at[s]), (sh_ref.at[s], sl_ref.at[s])],
        )
        xs, ys = plane_rows(cell_ref, tables, s, ALL)
        charges = -live_charges(charge_ref, count_ref, s, 0, ALL)
        xy_ref[s, :TALL, :] = xs[0]
        xy_ref[s, TALL : 2 * TALL, :] = xs[1]
        xy_ref[s, 2 * TALL : 2 * TALL + WIDE, :] = ys[0] * charges
        xy_ref[s, 2 * TALL + WIDE :, :] = ys[1] * charges


def side_weights(xy_ref, s, lanes):
    xy = xy_ref[s, :, lanes]
    return (
        (xy[:TALL], xy[TALL : 2 * TALL]),
        (xy[2 * TALL : 2 * TALL + WIDE], xy[2 * TALL + WIDE :]),
    )


def forward_z_kernel(mesh_ref, xr_ref, yr_ref, cr_ref, zc, out_ref, m):
    m[...] = mesh_ref[...]
    parts = []
    for s in range(2):
        base = (YB - RIM) * XB
        columns = []
        for h in range(2):
            k = 2 * s + h
            m[k, base : base + YRIM, :] += yr_ref[k]
            for x in range(RIM):
                rows = pl.ds(XB - RIM + x, YB, stride=XB)
                m[k, rows, :] += xr_ref[k, x * YB : x * YB + YB, :]
            for y in range(RIM):
                at = (YB - RIM + y) * XB + XB - 8
                m[k, at : at + 8, :] += cr_ref[k, y * 8 : y * 8 + 8]
            columns.append(m[k].T)
        parts.append(split(jnp.concatenate(columns, axis=0)))
    cosines, sines = (zc[0], zc[1]), (zc[2], zc[3])
    real = dot3(cosines, parts[0]) + dot3(sines, parts[1])
    imag = dot3(cosines, parts[1]) - dot3(sines, parts[0])
    for q, value in enumerate((real, imag)):
        for p in range(2):
            for b in range(4):
                out_ref[pl.ds(p * 8 + q * 4 + b, DEV, stride=16), :] = value[
                    p * DEV : (p + 1) * DEV, b * 128 : (b + 1) * 128
                ]


def exchange_blocks(pieces):
    lane = lax.broadcasted_iota(jnp.int32, pieces[0].shape, 1)
    for bit in (1, 2):
        upper = (lane // 32) & bit == bit
        fresh = list(pieces)
        for v in range(4):
            if v & bit == 0:
                a, b = pieces[v], pieces[v | bit]
                fresh[v] = jnp.where(upper, pltpu.roll(b, 32 * bit, 1), a)
                fresh[v | bit] = jnp.where(upper, b, pltpu.roll(a, 128 - 32 * bit, 1))
        pieces = fresh
    return pieces


def plane_kernel(buf_ref, green_ref, yc, xc, out_ref, d, o):
    cosines, sines = (xc[0], xc[1]), (xc[2], xc[3])
    planes = range(2)
    for p in planes:
        for c in range(COLS):
            for g in range(2):
                tiles = []
                for r in range(4):
                    at = ((g * 4 + r) * COLS + c) * 16 + p * 8
                    tiles.append(buf_ref[at : at + 8, :])
                for low, tile in enumerate(exchange_blocks(tiles)):
                    at = (c * 4 + low) * 8
                    d[p, at : at + 8, g * 128 : g * 128 + 128] = tile
    first = [dot3((yc[0], yc[1]), split(d[p])) for p in planes]
    parts = [(split(f[:K]), split(f[K:])) for f in first]
    parts = [
        (dot3(real, cosines) + dot3(imag, sines), dot3(imag, cosines) - dot3(real, sines))
        for real, imag in parts
    ]
    scaled = []
    for p in planes:
        green = jnp.concatenate(
            [green_ref[(r * 2 + p) * XB : (r * 2 + p + 1) * XB, :] for r in range(ROWS)], axis=0
        ) * (1.0 / float(K) ** 3)
        scaled.append([split(part * green) for part in parts[p]])
    parts = [
        (
            split(dot3(real, cosines) - dot3(imag, sines)),
            split(dot3(imag, cosines) + dot3(real, sines)),
        )
        for real, imag in scaled
    ]
    for p in planes:
        both = tuple(jnp.concatenate([a, b], axis=0) for a, b in zip(*parts[p]))
        o[p] = dot3((yc[2], yc[3]), both)
    for p in planes:
        for c in range(COLS):
            for g in range(2):
                tiles = []
                for low in range(4):
                    at = (c * 4 + low) * 8
                    tiles.append(o[p, at : at + 8, g * 128 : g * 128 + 128])
                for r, tile in enumerate(exchange_blocks(tiles)):
                    at = ((g * 4 + r) * COLS + c) * 16 + p * 8
                    out_ref[at : at + 8, :] = tile


def inverse_z_kernel(buf_ref, zc, fh_ref, fl_ref, xr_ref, yr_ref, cr_ref, m):
    cosines, sines = (zc[0], zc[1]), (zc[2], zc[3])
    parts = []
    for q in range(2):
        columns = []
        for p in range(2):
            blocks = []
            for b in range(4):
                blocks.append(buf_ref[pl.ds(p * 8 + q * 4 + b, DEV, stride=16), :].T)
            columns.append(jnp.concatenate(blocks, axis=0))
        parts.append(split(jnp.concatenate(columns, axis=1)))
    real, imag = parts
    fields = (
        dot3(real, cosines) - dot3(imag, sines),
        dot3(imag, cosines) + dot3(real, sines),
    )
    base = (YB - RIM) * XB
    for s in range(2):
        fh_ref[s], fl_ref[s] = split(fields[s])
        for h in range(2):
            k = 2 * s + h
            m[k] = fields[s][:, h * 128 : h * 128 + 128]
            yr_ref[k] = m[k, base : base + YRIM, :]
            for x in range(RIM):
                rows = pl.ds(XB - RIM + x, YB, stride=XB)
                xr_ref[k, x * YB : x * YB + YB, :] = m[k, rows, :]
            for y in range(RIM):
                at = (YB - RIM + y) * XB + XB - 8
                cr_ref[k, y * 8 : y * 8 + 8, :] = m[k, at : at + 8, :]


def row(pair, n):
    return pair[0][n : n + 1], pair[1][n : n + 1]


def weighed(plain, sloped, at, along, across):
    value, slope = across
    size = value.shape[0]
    sums = [None] * 3
    for n, (mine, mine_slope) in enumerate(along):
        rows = slice(at + n * size, at + (n + 1) * size)
        terms = (mine * plain[rows], mine_slope * plain[rows], mine * sloped[rows])
        sums = [term if n == 0 else old + term for old, term in zip(sums, terms)]
    return tuple(
        jnp.sum(total * side, axis=0, keepdims=True)
        for total, side in zip(sums, (slope, value, value))
    )


def chunks(body):
    def step(i, carry):
        at = pl.multiple_of(i * CHUNK, CHUNK)
        body(at, pl.ds(at, CHUNK))
        return carry

    lax.fori_loop(0, ATOMS // CHUNK, step, 0)


def gather_kernel(xy_ref, wh_ref, wl_ref, sh_ref, sl_ref, fh_ref, fl_ref, out_ref):
    def body(at, lanes):
        for s in range(2):
            xs, ys = side_weights(xy_ref, s, lanes)
            field = fh_ref[s], fl_ref[s]
            plain = dot3(field, (wh_ref[s, :, lanes], wl_ref[s, :, lanes]))
            sloped = dot3(field, (sh_ref[s, :, lanes], sl_ref[s, :, lanes]))
            lines = [row(ys, 8 + y) for y in range(YB)]
            forces = weighed(plain, sloped, 0, lines, (xs[0][8:], xs[1][8:]))
            for d in range(3):
                out_ref[d, s : s + 1, lanes] = forces[d]

    chunks(body)


def gather_rim_kernel(
    xy_ref, wh_ref, wl_ref, sh_ref, sl_ref, xr_ref, yr_ref, cr_ref, inner_ref, out_ref, fh, fl,
):
    for s in range(2):
        for h in range(2):
            k, columns = 2 * s + h, slice(h * 128, h * 128 + 128)
            corner = jnp.concatenate([cr_ref[k], jnp.zeros((8, 128), F32)], axis=0)
            for value, at in ((xr_ref[k], 0), (yr_ref[k], XRIM), (corner, XRIM + YRIM)):
                top, rest = split(value)
                fh[s, at : at + value.shape[0], columns] = top
                fl[s, at : at + value.shape[0], columns] = rest

    def body(at, lanes):
        for s in range(2):
            xs, ys = side_weights(xy_ref, s, lanes)
            field = fh[s], fl[s]
            plain = dot3(field, (wh_ref[s, :, lanes], wl_ref[s, :, lanes]))
            sloped = dot3(field, (sh_ref[s, :, lanes], sl_ref[s, :, lanes]))
            lines = [row(ys, 3 + y) for y in range(RIM)]
            columns = [row(xs, 3 + x) for x in range(RIM)]
            side = weighed(plain, sloped, 0, columns, (ys[0][8:], ys[1][8:]))
            edge = weighed(plain, sloped, XRIM, lines, (xs[0][8:], xs[1][8:]))
            corner = weighed(plain, sloped, XRIM + YRIM, lines, (xs[0][:8], xs[1][:8]))
            for d, e in ((0, 1), (1, 0), (2, 2)):
                force = inner_ref[d, s : s + 1, lanes] + side[e] + edge[d] + corner[d]
                out_ref[d, s : s + 1, lanes] = force

    chunks(body)


def green_kernel(in_ref, out_ref, m):
    for h in range(2):
        lanes = slice(h * 128, h * 128 + 128)
        m[...] = in_ref[:, lanes]
        for k in range(COLS):
            out_ref[k * XB : (k + 1) * XB, lanes] = m[pl.ds(k, XB, stride=COLS), :]


def call(kernel, name, flops, out_shape, operands, smem=(), hbm=(), scratch=(), limit=24):
    def spec(n):
        if n in hbm:
            return HBM_ALL
        return SMEM_ALL if n in smem else VMEM_ALL

    single = not isinstance(out_shape, list)
    shapes = [out_shape] if single else out_shape
    size = sum(math.prod(v.shape) * v.dtype.itemsize for v in list(operands) + shapes)
    return pl.pallas_call(
        kernel,
        out_shape=out_shape,
        in_specs=[spec(n) for n in range(len(operands))],
        out_specs=VMEM_ALL if single else [VMEM_ALL] * len(shapes),
        scratch_shapes=list(scratch),
        compiler_params=pltpu.CompilerParams(vmem_limit_bytes=limit * 2**20),
        cost_estimate=pl.CostEstimate(flops=int(flops), bytes_accessed=size, transcendentals=0),
        name=name,
    )(*operands)


def shape(*dims, dtype=F32):
    return jax.ShapeDtypeStruct(dims, dtype)


def shift(value, rows, cols):
    pairs = []
    for r in range(ROWS):
        for c in range(COLS):
            pairs.append((r * COLS + c, ((r + rows) % ROWS) * COLS + (c + cols) % COLS))
    return lax.ppermute(value, ("row", "col"), pairs)


def everywhere(value):
    return lax.all_to_all(value, ("row", "col"), split_axis=0, concat_axis=0, tiled=True)


def shards(cell_index, fraction, charge, atom_count, influence):
    zc = jnp.asarray(z_tables())
    xc = jnp.asarray(x_tables())
    table = y_table()
    yc = jnp.asarray(np.stack(halves(table) + halves(np.ascontiguousarray(table.T))))

    cells = jnp.transpose(cell_index, (1, 0, 2))
    fractions = jnp.transpose(fraction, (1, 0, 2))
    counts = jnp.transpose(atom_count, (1, 0))
    atoms = (counts, cells, fractions, charge)
    rim_shapes = [shape(4, XRIM, 128), shape(4, YRIM, 128), shape(4, CRIM, 128)]
    weights = shape(2, K, ATOMS, dtype=BF16)

    table = pltpu.VMEM((2, K, ATOMS), BF16)
    xr, yr, cr = call(
        spread_rim_kernel, "spread_rim", 6e9, rim_shapes, atoms,
        smem=(0,), hbm=(1, 2, 3), limit=60,
        scratch=[
            pltpu.VMEM((3, 2, ATOMS), jnp.int32),
            pltpu.VMEM((3, 2, ATOMS), F32),
            pltpu.VMEM((2, ATOMS), F32),
            pltpu.VMEM((2, RIMS + 8, ATOMS), BF16),
            pltpu.VMEM((2, RIMS + 8, ATOMS), BF16),
            table,
            table,
            pltpu.SemaphoreType.DMA((3,)),
        ],
    )
    later, _ = lax.optimization_barrier((influence, cr))
    xr, yr, cr = shift(xr, -1, 0), shift(yr, 0, -1), shift(cr, -1, -1)
    green = call(
        green_kernel, "green", 1e8, shape(512, K), (later.reshape(XB * COLS, K),),
        scratch=[pltpu.VMEM((512, 128), F32)],
    )
    green = lax.all_to_all(
        green.reshape(ROWS, 64, K), "row", split_axis=0, concat_axis=0, tiled=True
    ).reshape(512, K)
    mesh = call(
        spread_kernel, "spread", 8e9, shape(4, INNER, 128), atoms,
        smem=(0,), limit=32,
        scratch=[pltpu.VMEM((2, INNER, ATOMS), BF16)] * 2 + [table] * 2,
    )
    packed = call(
        forward_z_kernel, "forward_z", 3e9, shape(DEV * 16, 128), (mesh, xr, yr, cr, zc),
        scratch=[pltpu.VMEM((4, INNER, 128), F32)],
    )
    packed = everywhere(packed.reshape(DEV, 16, 128)).reshape(DEV * 16, 128)
    wh, wl, gh, gl, xy = call(
        weight_kernel, "weights", 1e10, [weights] * 4 + [shape(2, SIDES, ATOMS)], atoms, smem=(0,)
    )
    packed = call(
        plane_kernel, "planes", 6e9, shape(DEV * 16, 128), (packed, green, yc, xc),
        scratch=[pltpu.VMEM((2, 512, K), F32)] * 2,
    )
    packed = everywhere(packed.reshape(DEV, 16, 128)).reshape(DEV * 16, 128)
    fh, fl, xr, yr, cr = call(
        inverse_z_kernel, "inverse_z", 3e9, [shape(2, INNER, K, dtype=BF16)] * 2 + rim_shapes,
        (packed, zc),
        scratch=[pltpu.VMEM((4, INNER, 128), F32)],
    )
    xr, yr, cr = shift(xr, 1, 0), shift(yr, 0, 1), shift(cr, 1, 1)
    inner = call(
        gather_kernel, "gather", 1.2e10, shape(3, 2, ATOMS),
        (xy, wh, wl, gh, gl, fh, fl),
    )
    forces = call(
        gather_rim_kernel, "gather_rim", 8e9, shape(3, 2, ATOMS),
        (xy, wh, wl, gh, gl, xr, yr, cr, inner),
        scratch=[pltpu.VMEM((2, RIMS + 8, K), BF16)] * 2,
    )
    return jnp.transpose(forces, (1, 0, 2))


def solution(mesh):
    placed = (
        P(None, None, ("row", "col")),
        P(None, None, ("row", "col")),
        P(None, ("row", "col")),
        P(None, ("row", "col")),
        P("row", "col", None),
    )
    return jax.shard_map(
        shards, mesh=mesh, in_specs=placed, out_specs=P(None, None, ("row", "col")), check_vma=False
    )
```

```python
import math

import jax
import jax.numpy as jnp
import numpy as np
from jax import lax
from jax.experimental import pallas as pl
from jax.experimental.pallas import tpu as pltpu
from jax.sharding import PartitionSpec as P

F32 = jnp.float32
BF16 = jnp.bfloat16
K = 256
XB = 32
YB = 16
ROWS = 8
COLS = 16
DEV = ROWS * COLS
ATOMS = 2048
CHUNK = 512
RIM = 5
INNER = XB * YB
XRIM = RIM * YB
YRIM = RIM * XB
CRIM = RIM * 8
RIMS = XRIM + YRIM + CRIM
VMEM_ALL = pl.BlockSpec(memory_space=pltpu.VMEM)
HBM_ALL = pl.BlockSpec(memory_space=pltpu.HBM)
SMEM_ALL = pl.BlockSpec(memory_space=pltpu.SMEM)


def halves(values):
    top = values.astype(np.float32).astype(jnp.bfloat16)
    rest = (values - top.astype(np.float64)).astype(np.float32).astype(jnp.bfloat16)
    return top, rest


def z_tables():
    p, d = np.meshgrid(np.arange(2), np.arange(DEV), indexing="ij")
    kz = (16 * (d % COLS) + 2 * (d // COLS) + p).reshape(-1)
    angle = 2.0 * math.pi * ((kz[:, None] * np.arange(K)[None, :]) % K) / K
    return np.stack(halves(np.cos(angle)) + halves(np.sin(angle)))


def x_tables():
    x = np.arange(K)
    angle = 2.0 * math.pi * ((x[:, None] * x[None, :]) % K) / K
    return np.stack(halves(np.cos(angle)) + halves(np.sin(angle)))


def y_table():
    c, low, part, high = np.meshgrid(
        np.arange(COLS), np.arange(4), np.arange(2), np.arange(4), indexing="ij"
    )
    y = (16 * c + 4 * high + low).reshape(-1)
    part = part.reshape(-1)[None, :]
    angle = 2.0 * math.pi * ((np.arange(K)[:, None] * y[None, :]) % K) / K
    cosine, sine = np.cos(angle), np.sin(angle)
    real = np.where(part == 0, cosine, sine)
    imag = np.where(part == 0, -sine, cosine)
    return np.concatenate([real, imag], axis=0)


def split(value):
    top = value.astype(BF16)
    return top, (value - top.astype(F32)).astype(BF16)


def dot(a, b, dims=((1,), (0,))):
    return lax.dot_general(a, b, (dims, ((), ())), preferred_element_type=F32)


def dot3(a, b, dims=((1,), (0,))):
    return dot(a[0], b[0], dims) + dot(a[0], b[1], dims) + dot(a[1], b[0], dims)


def spline_values(fraction):
    nothing = jnp.zeros_like(fraction)
    levels = [fraction, 1.0 - fraction]
    slopes = levels
    for degree in range(3, 7):
        padded = levels + [nothing]
        following = []
        for offset in range(degree):
            beneath = padded[offset - 1] if offset > 0 else nothing
            following.append(
                ((fraction + offset) * padded[offset] + (degree - fraction - offset) * beneath)
                * (1.0 / (degree - 1))
            )
        if degree == 6:
            slopes = [
                padded[offset] - (padded[offset - 1] if offset > 0 else nothing)
                for offset in range(6)
            ]
        levels = following
    return levels, slopes


def placed_rows(cell, values, first, count, wrapped):
    shape = (count, cell.shape[1])
    behind = cell - (lax.broadcasted_iota(jnp.int32, shape, 0) + first)
    if wrapped:
        behind = behind & (K - 1)
    masks = [behind == j for j in range(6)]
    results = []
    for value in values:
        total = jnp.zeros(shape, F32)
        for j in range(6):
            total = jnp.where(masks[j], value[j], total)
        results.append(total)
    return results


def place_tables(cell, values, outs):
    count = cell.shape[1]
    base = (cell - lax.broadcasted_iota(jnp.int32, (16, count), 0)).astype(jnp.int16)
    parts = []
    for value in values:
        rows = [split(jnp.broadcast_to(value[j], (16, count))) for j in range(6)]
        parts.append(([row[0] for row in rows], [row[1] for row in rows]))
    for g in range(K // 16):
        behind = (base - jnp.int16(16 * g)) & jnp.int16(K - 1)
        results = [[jnp.zeros((16, count), BF16)] * 2 for _ in values]
        for j in range(6):
            mask = behind == jnp.int16(j)
            results = [
                [jnp.where(mask, part[n][j], result[n]) for n in range(2)]
                for part, result in zip(parts, results)
            ]
        for result, out in zip(results, outs):
            for n in range(2):
                out[n][g * 16 : g * 16 + 16, :] = result[n]


def atom_rows(frac_ref, lanes):
    fraction = jnp.concatenate([frac_ref[d, :, lanes] for d in range(3)], axis=0)
    return spline_values(fraction)


def live_charges(charge_ref, count_ref, s, at, lanes):
    slots = lax.broadcasted_iota(jnp.int32, (1, lanes.size), 1) + at
    return jnp.where(slots < count_ref[0, s], charge_ref[s : s + 1, lanes], 0.0)


def pick(rows, d, s):
    return [w[2 * d + s : 2 * d + s + 1] for w in rows]


def plane_rows(cell_ref, tables, s, lanes):
    first = cell_ref[0, s : s + 1, lanes] & (XB - 1)
    second = cell_ref[1, s : s + 1, lanes] & (YB - 1)
    return (
        placed_rows(first, [pick(t, 0, s) for t in tables], -8, XB + 8, False),
        placed_rows(second, [pick(t, 1, s) for t in tables], -8, YB + 8, False),
    )


def put(ph, pq, at, product):
    top, rest = split(product)
    ph[at : at + product.shape[0], :] = top
    pq[at : at + product.shape[0], :] = rest


ALL = pl.ds(0, ATOMS)


def give(total, s, pieces):
    for ref, at, count in pieces:
        for h in range(2):
            ref[2 * s + h] = total[at : at + count, h * 128 : h * 128 + 128]


def spread_rim_kernel(
    count_ref, cell_hbm, frac_hbm, charge_hbm, xr_ref, yr_ref, cr_ref,
    cell_ref, frac_ref, charge_ref, ph, pq, wh_ref, wl_ref, sems,
):
    copies = [
        pltpu.make_async_copy(source, target, sems.at[n])
        for n, (source, target) in enumerate(
            ((cell_hbm, cell_ref), (frac_hbm, frac_ref), (charge_hbm, charge_ref))
        )
    ]
    for copy in copies:
        copy.start()
    for copy in copies:
        copy.wait()
    levels, _ = atom_rows(frac_ref, ALL)
    for s in range(2):
        (first,), (second,) = plane_rows(cell_ref, [levels], s, ALL)
        place_tables(cell_ref[2, s : s + 1, :], [pick(levels, 2, s)], [(wh_ref.at[s], wl_ref.at[s])])
        second = second * live_charges(charge_ref, count_ref, s, 0, ALL)
        p, q = ph.at[s], pq.at[s]
        for x in range(RIM):
            put(p, q, x * YB, first[3 + x : 4 + x] * second[8:])
        for y in range(RIM):
            put(p, q, XRIM + y * XB, second[3 + y : 4 + y] * first[8:])
        corner = [second[3 + y : 4 + y] * first[:8] for y in range(RIM)]
        corner.append(jnp.zeros((8, ATOMS), F32))
        for y in range(0, RIM + 1, 2):
            put(p, q, XRIM + YRIM + y * 8, jnp.concatenate(corner[y : y + 2], axis=0))
        total = dot3((p[...], q[...]), (wh_ref[s], wl_ref[s]), ((1,), (1,)))
        give(total, s, ((xr_ref, 0, XRIM), (yr_ref, XRIM, YRIM), (cr_ref, XRIM + YRIM, CRIM)))


def spread_kernel(count_ref, cell_ref, frac_ref, charge_ref, mesh_ref, ph, pq, wh_ref, wl_ref):
    levels, _ = atom_rows(frac_ref, ALL)
    for s in range(2):
        (first,), (second,) = plane_rows(cell_ref, [levels], s, ALL)
        second = second * live_charges(charge_ref, count_ref, s, 0, ALL)
        place_tables(cell_ref[2, s : s + 1, :], [pick(levels, 2, s)], [(wh_ref.at[s], wl_ref.at[s])])
        p, q = ph.at[s], pq.at[s]
        for y in range(YB):
            put(p, q, y * XB, second[8 + y : 9 + y] * first[8:])
        total = dot3((p[...], q[...]), (wh_ref[s], wl_ref[s]), ((1,), (1,)))
        give(total, s, ((mesh_ref, 0, INNER),))


TALL, WIDE = XB + 8, YB + 8
SIDES = 2 * TALL + 2 * WIDE


def weight_kernel(count_ref, cell_ref, frac_ref, charge_ref, wh_ref, wl_ref, sh_ref, sl_ref, xy_ref):
    tables = atom_rows(frac_ref, ALL)
    for s in range(2):
        place_tables(
            cell_ref[2, s : s + 1, :],
            [pick(t, 2, s) for t in tables],
            [(wh_ref.at[s], wl_ref.at[s]), (sh_ref.at[s], sl_ref.at[s])],
        )
        xs, ys = plane_rows(cell_ref, tables, s, ALL)
        charges = -live_charges(charge_ref, count_ref, s, 0, ALL)
        xy_ref[s, :TALL, :] = xs[0]
        xy_ref[s, TALL : 2 * TALL, :] = xs[1]
        xy_ref[s, 2 * TALL : 2 * TALL + WIDE, :] = ys[0] * charges
        xy_ref[s, 2 * TALL + WIDE :, :] = ys[1] * charges


def side_weights(xy_ref, s, lanes):
    xy = xy_ref[s, :, lanes]
    return (
        (xy[:TALL], xy[TALL : 2 * TALL]),
        (xy[2 * TALL : 2 * TALL + WIDE], xy[2 * TALL + WIDE :]),
    )


def forward_z_kernel(mesh_ref, xr_ref, yr_ref, cr_ref, zc, out_ref, m):
    m[...] = mesh_ref[...]
    parts = []
    for s in range(2):
        base = (YB - RIM) * XB
        columns = []
        for h in range(2):
            k = 2 * s + h
            m[k, base : base + YRIM, :] += yr_ref[k]
            for x in range(RIM):
                rows = pl.ds(XB - RIM + x, YB, stride=XB)
                m[k, rows, :] += xr_ref[k, x * YB : x * YB + YB, :]
            for y in range(RIM):
                at = (YB - RIM + y) * XB + XB - 8
                m[k, at : at + 8, :] += cr_ref[k, y * 8 : y * 8 + 8]
            columns.append(m[k].T)
        parts.append(split(jnp.concatenate(columns, axis=0)))
    cosines, sines = (zc[0], zc[1]), (zc[2], zc[3])
    real = dot3(cosines, parts[0]) + dot3(sines, parts[1])
    imag = dot3(cosines, parts[1]) - dot3(sines, parts[0])
    for q, value in enumerate((real, imag)):
        for p in range(2):
            for b in range(4):
                out_ref[pl.ds(p * 8 + q * 4 + b, DEV, stride=16), :] = value[
                    p * DEV : (p + 1) * DEV, b * 128 : (b + 1) * 128
                ]


def exchange_blocks(pieces):
    lane = lax.broadcasted_iota(jnp.int32, pieces[0].shape, 1)
    for bit in (1, 2):
        upper = (lane // 32) & bit == bit
        fresh = list(pieces)
        for v in range(4):
            if v & bit == 0:
                a, b = pieces[v], pieces[v | bit]
                fresh[v] = jnp.where(upper, pltpu.roll(b, 32 * bit, 1), a)
                fresh[v | bit] = jnp.where(upper, b, pltpu.roll(a, 128 - 32 * bit, 1))
        pieces = fresh
    return pieces


def plane_kernel(buf_ref, green_ref, yc, xc, out_ref, d, o):
    cosines, sines = (xc[0], xc[1]), (xc[2], xc[3])
    planes = range(2)
    for p in planes:
        for c in range(COLS):
            for g in range(2):
                tiles = []
                for r in range(4):
                    at = ((g * 4 + r) * COLS + c) * 16 + p * 8
                    tiles.append(buf_ref[at : at + 8, :])
                for low, tile in enumerate(exchange_blocks(tiles)):
                    at = (c * 4 + low) * 8
                    d[p, at : at + 8, g * 128 : g * 128 + 128] = tile
    first = [dot3((yc[0], yc[1]), split(d[p])) for p in planes]
    parts = [(split(f[:K]), split(f[K:])) for f in first]
    parts = [
        (dot3(real, cosines) + dot3(imag, sines), dot3(imag, cosines) - dot3(real, sines))
        for real, imag in parts
    ]
    scaled = []
    for p in planes:
        green = jnp.concatenate(
            [green_ref[(r * 2 + p) * XB : (r * 2 + p + 1) * XB, :] for r in range(ROWS)], axis=0
        ) * (1.0 / float(K) ** 3)
        scaled.append([split(part * green) for part in parts[p]])
    parts = [
        (
            split(dot3(real, cosines) - dot3(imag, sines)),
            split(dot3(imag, cosines) + dot3(real, sines)),
        )
        for real, imag in scaled
    ]
    for p in planes:
        both = tuple(jnp.concatenate([a, b], axis=0) for a, b in zip(*parts[p]))
        o[p] = dot3((yc[2], yc[3]), both)
    for p in planes:
        for c in range(COLS):
            for g in range(2):
                tiles = []
                for low in range(4):
                    at = (c * 4 + low) * 8
                    tiles.append(o[p, at : at + 8, g * 128 : g * 128 + 128])
                for r, tile in enumerate(exchange_blocks(tiles)):
                    at = ((g * 4 + r) * COLS + c) * 16 + p * 8
                    out_ref[at : at + 8, :] = tile


def inverse_z_kernel(buf_ref, zc, fh_ref, fl_ref, xr_ref, yr_ref, cr_ref, m):
    cosines, sines = (zc[0], zc[1]), (zc[2], zc[3])
    parts = []
    for q in range(2):
        columns = []
        for p in range(2):
            blocks = []
            for b in range(4):
                blocks.append(buf_ref[pl.ds(p * 8 + q * 4 + b, DEV, stride=16), :].T)
            columns.append(jnp.concatenate(blocks, axis=0))
        parts.append(split(jnp.concatenate(columns, axis=1)))
    real, imag = parts
    fields = (
        dot3(real, cosines) - dot3(imag, sines),
        dot3(imag, cosines) + dot3(real, sines),
    )
    base = (YB - RIM) * XB
    for s in range(2):
        fh_ref[s], fl_ref[s] = split(fields[s])
        for h in range(2):
            k = 2 * s + h
            m[k] = fields[s][:, h * 128 : h * 128 + 128]
            yr_ref[k] = m[k, base : base + YRIM, :]
            for x in range(RIM):
                rows = pl.ds(XB - RIM + x, YB, stride=XB)
                xr_ref[k, x * YB : x * YB + YB, :] = m[k, rows, :]
            for y in range(RIM):
                at = (YB - RIM + y) * XB + XB - 8
                cr_ref[k, y * 8 : y * 8 + 8, :] = m[k, at : at + 8, :]


def row(pair, n):
    return pair[0][n : n + 1], pair[1][n : n + 1]


def weighed(plain, sloped, at, along, across):
    value, slope = across
    size = value.shape[0]
    sums = [None] * 3
    for n, (mine, mine_slope) in enumerate(along):
        rows = slice(at + n * size, at + (n + 1) * size)
        terms = (mine * plain[rows], mine_slope * plain[rows], mine * sloped[rows])
        sums = [term if n == 0 else old + term for old, term in zip(sums, terms)]
    return tuple(
        jnp.sum(total * side, axis=0, keepdims=True)
        for total, side in zip(sums, (slope, value, value))
    )


def chunks(body):
    def step(i, carry):
        at = pl.multiple_of(i * CHUNK, CHUNK)
        body(at, pl.ds(at, CHUNK))
        return carry

    lax.fori_loop(0, ATOMS // CHUNK, step, 0, unroll=2)


def gather_kernel(xy_ref, wh_ref, wl_ref, sh_ref, sl_ref, fh_ref, fl_ref, out_ref):
    def body(at, lanes):
        for s in range(2):
            xs, ys = side_weights(xy_ref, s, lanes)
            field = fh_ref[s], fl_ref[s]
            plain = dot3(field, (wh_ref[s, :, lanes], wl_ref[s, :, lanes]))
            sloped = dot3(field, (sh_ref[s, :, lanes], sl_ref[s, :, lanes]))
            lines = [row(ys, 8 + y) for y in range(YB)]
            forces = weighed(plain, sloped, 0, lines, (xs[0][8:], xs[1][8:]))
            for d in range(3):
                out_ref[d, s : s + 1, lanes] = forces[d]

    chunks(body)


def gather_rim_kernel(
    xy_ref, wh_ref, wl_ref, sh_ref, sl_ref, xr_ref, yr_ref, cr_ref, inner_ref, out_ref, fh, fl,
):
    for s in range(2):
        for h in range(2):
            k, columns = 2 * s + h, slice(h * 128, h * 128 + 128)
            corner = jnp.concatenate([cr_ref[k], jnp.zeros((8, 128), F32)], axis=0)
            for value, at in ((xr_ref[k], 0), (yr_ref[k], XRIM), (corner, XRIM + YRIM)):
                top, rest = split(value)
                fh[s, at : at + value.shape[0], columns] = top
                fl[s, at : at + value.shape[0], columns] = rest

    def body(at, lanes):
        for s in range(2):
            xs, ys = side_weights(xy_ref, s, lanes)
            field = fh[s], fl[s]
            plain = dot3(field, (wh_ref[s, :, lanes], wl_ref[s, :, lanes]))
            sloped = dot3(field, (sh_ref[s, :, lanes], sl_ref[s, :, lanes]))
            lines = [row(ys, 3 + y) for y in range(RIM)]
            columns = [row(xs, 3 + x) for x in range(RIM)]
            side = weighed(plain, sloped, 0, columns, (ys[0][8:], ys[1][8:]))
            edge = weighed(plain, sloped, XRIM, lines, (xs[0][8:], xs[1][8:]))
            corner = weighed(plain, sloped, XRIM + YRIM, lines, (xs[0][:8], xs[1][:8]))
            for d, e in ((0, 1), (1, 0), (2, 2)):
                force = inner_ref[d, s : s + 1, lanes] + side[e] + edge[d] + corner[d]
                out_ref[d, s : s + 1, lanes] = force

    chunks(body)


def green_kernel(in_ref, out_ref, m):
    for h in range(2):
        lanes = slice(h * 128, h * 128 + 128)
        m[...] = in_ref[:, lanes]
        for k in range(COLS):
            out_ref[k * XB : (k + 1) * XB, lanes] = m[pl.ds(k, XB, stride=COLS), :]


def call(kernel, name, flops, out_shape, operands, smem=(), hbm=(), scratch=(), limit=24):
    def spec(n):
        if n in hbm:
            return HBM_ALL
        return SMEM_ALL if n in smem else VMEM_ALL

    single = not isinstance(out_shape, list)
    shapes = [out_shape] if single else out_shape
    size = sum(math.prod(v.shape) * v.dtype.itemsize for v in list(operands) + shapes)
    return pl.pallas_call(
        kernel,
        out_shape=out_shape,
        in_specs=[spec(n) for n in range(len(operands))],
        out_specs=VMEM_ALL if single else [VMEM_ALL] * len(shapes),
        scratch_shapes=list(scratch),
        compiler_params=pltpu.CompilerParams(vmem_limit_bytes=limit * 2**20),
        cost_estimate=pl.CostEstimate(flops=int(flops), bytes_accessed=size, transcendentals=0),
        name=name,
    )(*operands)


def shape(*dims, dtype=F32):
    return jax.ShapeDtypeStruct(dims, dtype)


def shift(value, rows, cols):
    pairs = []
    for r in range(ROWS):
        for c in range(COLS):
            pairs.append((r * COLS + c, ((r + rows) % ROWS) * COLS + (c + cols) % COLS))
    return lax.ppermute(value, ("row", "col"), pairs)


def everywhere(value):
    return lax.all_to_all(value, ("row", "col"), split_axis=0, concat_axis=0, tiled=True)


def shards(cell_index, fraction, charge, atom_count, influence):
    zc = jnp.asarray(z_tables())
    xc = jnp.asarray(x_tables())
    table = y_table()
    yc = jnp.asarray(np.stack(halves(table) + halves(np.ascontiguousarray(table.T))))

    cells = jnp.transpose(cell_index, (1, 0, 2))
    fractions = jnp.transpose(fraction, (1, 0, 2))
    counts = jnp.transpose(atom_count, (1, 0))
    atoms = (counts, cells, fractions, charge)
    rim_shapes = [shape(4, XRIM, 128), shape(4, YRIM, 128), shape(4, CRIM, 128)]
    weights = shape(2, K, ATOMS, dtype=BF16)

    table = pltpu.VMEM((2, K, ATOMS), BF16)
    xr, yr, cr = call(
        spread_rim_kernel, "spread_rim", 6e9, rim_shapes, atoms,
        smem=(0,), hbm=(1, 2, 3), limit=60,
        scratch=[
            pltpu.VMEM((3, 2, ATOMS), jnp.int32),
            pltpu.VMEM((3, 2, ATOMS), F32),
            pltpu.VMEM((2, ATOMS), F32),
            pltpu.VMEM((2, RIMS + 8, ATOMS), BF16),
            pltpu.VMEM((2, RIMS + 8, ATOMS), BF16),
            table,
            table,
            pltpu.SemaphoreType.DMA((3,)),
        ],
    )
    later, _ = lax.optimization_barrier((influence, cr))
    xr, yr, cr = shift(xr, -1, 0), shift(yr, 0, -1), shift(cr, -1, -1)
    green = call(
        green_kernel, "green", 1e8, shape(512, K), (later.reshape(XB * COLS, K),),
        scratch=[pltpu.VMEM((512, 128), F32)],
    )
    green = lax.all_to_all(
        green.reshape(ROWS, 64, K), "row", split_axis=0, concat_axis=0, tiled=True
    ).reshape(512, K)
    mesh = call(
        spread_kernel, "spread", 8e9, shape(4, INNER, 128), atoms,
        smem=(0,), limit=32,
        scratch=[pltpu.VMEM((2, INNER, ATOMS), BF16)] * 2 + [table] * 2,
    )
    packed = call(
        forward_z_kernel, "forward_z", 3e9, shape(DEV * 16, 128), (mesh, xr, yr, cr, zc),
        scratch=[pltpu.VMEM((4, INNER, 128), F32)],
    )
    packed = everywhere(packed.reshape(DEV, 16, 128)).reshape(DEV * 16, 128)
    wh, wl, gh, gl, xy = call(
        weight_kernel, "weights", 1e10, [weights] * 4 + [shape(2, SIDES, ATOMS)], atoms, smem=(0,),
        limit=60,
    )
    packed = call(
        plane_kernel, "planes", 6e9, shape(DEV * 16, 128), (packed, green, yc, xc),
        scratch=[pltpu.VMEM((2, 512, K), F32)] * 2,
    )
    packed = everywhere(packed.reshape(DEV, 16, 128)).reshape(DEV * 16, 128)
    fh, fl, xr, yr, cr = call(
        inverse_z_kernel, "inverse_z", 3e9, [shape(2, INNER, K, dtype=BF16)] * 2 + rim_shapes,
        (packed, zc),
        scratch=[pltpu.VMEM((4, INNER, 128), F32)],
    )
    xr, yr, cr = shift(xr, 1, 0), shift(yr, 0, 1), shift(cr, 1, 1)
    inner = call(
        gather_kernel, "gather", 1.2e10, shape(3, 2, ATOMS),
        (xy, wh, wl, gh, gl, fh, fl),
    )
    forces = call(
        gather_rim_kernel, "gather_rim", 8e9, shape(3, 2, ATOMS),
        (xy, wh, wl, gh, gl, xr, yr, cr, inner),
        scratch=[pltpu.VMEM((2, RIMS + 8, K), BF16)] * 2,
    )
    return jnp.transpose(forces, (1, 0, 2))


def solution(mesh):
    placed = (
        P(None, None, ("row", "col")),
        P(None, None, ("row", "col")),
        P(None, ("row", "col")),
        P(None, ("row", "col")),
        P("row", "col", None),
    )
    return jax.shard_map(
        shards, mesh=mesh, in_specs=placed, out_specs=P(None, None, ("row", "col")), check_vma=False
    )
```

```python
import math

import jax
import jax.numpy as jnp
import numpy as np
from jax import lax
from jax.experimental import pallas as pl
from jax.experimental.pallas import tpu as pltpu
from jax.sharding import PartitionSpec as P


F32 = jnp.float32
BF16 = jnp.bfloat16
K = 256
XB = 32
YB = 16
ROWS = 8
COLS = 16
DEV = ROWS * COLS
ATOMS = 2048
CHUNK = 512
RIM = 5
INNER = XB * YB
XRIM = RIM * YB
YRIM = RIM * XB
CRIM = RIM * 8
RIMS = XRIM + YRIM + CRIM
VMEM_ALL = pl.BlockSpec(memory_space=pltpu.VMEM)
HBM_ALL = pl.BlockSpec(memory_space=pltpu.HBM)
SMEM_ALL = pl.BlockSpec(memory_space=pltpu.SMEM)


def halves(values):
    top = values.astype(np.float32).astype(jnp.bfloat16)
    rest = (values - top.astype(np.float64)).astype(np.float32).astype(jnp.bfloat16)
    return top, rest


def z_tables():
    p, d = np.meshgrid(np.arange(2), np.arange(DEV), indexing="ij")
    kz = (16 * (d % COLS) + 2 * (d // COLS) + p).reshape(-1)
    angle = 2.0 * math.pi * ((kz[:, None] * np.arange(K)[None, :]) % K) / K
    return np.stack(halves(np.cos(angle)) + halves(np.sin(angle)))


def x_tables():
    x = np.arange(K)
    angle = 2.0 * math.pi * ((x[:, None] * x[None, :]) % K) / K
    return np.stack(halves(np.cos(angle)) + halves(np.sin(angle)))


def y_table():
    c, low, part, high = np.meshgrid(
        np.arange(COLS), np.arange(4), np.arange(2), np.arange(4), indexing="ij"
    )
    y = (16 * c + 4 * high + low).reshape(-1)
    part = part.reshape(-1)[None, :]
    angle = 2.0 * math.pi * ((np.arange(K)[:, None] * y[None, :]) % K) / K
    cosine, sine = np.cos(angle), np.sin(angle)
    real = np.where(part == 0, cosine, sine)
    imag = np.where(part == 0, -sine, cosine)
    return np.concatenate([real, imag], axis=0)


def split(value):
    top = value.astype(BF16)
    return top, (value - top.astype(F32)).astype(BF16)


def dot(a, b, dims=((1,), (0,))):
    return lax.dot_general(a, b, (dims, ((), ())), preferred_element_type=F32)


def dot3(a, b, dims=((1,), (0,))):
    return dot(a[0], b[0], dims) + dot(a[0], b[1], dims) + dot(a[1], b[0], dims)


def spline_values(fraction):
    nothing = jnp.zeros_like(fraction)
    levels = [fraction, 1.0 - fraction]
    slopes = levels
    for degree in range(3, 7):
        padded = levels + [nothing]
        following = []
        for offset in range(degree):
            beneath = padded[offset - 1] if offset > 0 else nothing
            following.append(
                ((fraction + offset) * padded[offset] + (degree - fraction - offset) * beneath)
                * (1.0 / (degree - 1))
            )
        if degree == 6:
            slopes = [
                padded[offset] - (padded[offset - 1] if offset > 0 else nothing)
                for offset in range(6)
            ]
        levels = following
    return levels, slopes


def placed_rows(cell, values, first, count, wrapped):
    shape = (count, cell.shape[1])
    behind = cell - (lax.broadcasted_iota(jnp.int32, shape, 0) + first)
    if wrapped:
        behind = behind & (K - 1)
    masks = [behind == j for j in range(6)]
    results = []
    for value in values:
        total = jnp.zeros(shape, F32)
        for j in range(6):
            total = jnp.where(masks[j], value[j], total)
        results.append(total)
    return results


def place_tables(cell, values, outs):
    count = cell.shape[1]
    base = (cell - lax.broadcasted_iota(jnp.int32, (16, count), 0)).astype(jnp.int16)
    parts = []
    for value in values:
        rows = [split(jnp.broadcast_to(value[j], (16, count))) for j in range(6)]
        parts.append(([row[0] for row in rows], [row[1] for row in rows]))
    for g in range(K // 16):
        behind = (base - jnp.int16(16 * g)) & jnp.int16(K - 1)
        results = [[jnp.zeros((16, count), BF16)] * 2 for _ in values]
        for j in range(6):
            mask = behind == jnp.int16(j)
            results = [
                [jnp.where(mask, part[n][j], result[n]) for n in range(2)]
                for part, result in zip(parts, results)
            ]
        for result, out in zip(results, outs):
            for n in range(2):
                out[n][g * 16 : g * 16 + 16, :] = result[n]


def atom_rows(frac_ref, lanes):
    fraction = jnp.concatenate([frac_ref[d, :, lanes] for d in range(3)], axis=0)
    return spline_values(fraction)


def live_charges(charge_ref, count_ref, s, at, lanes):
    slots = lax.broadcasted_iota(jnp.int32, (1, lanes.size), 1) + at
    return jnp.where(slots < count_ref[0, s], charge_ref[s : s + 1, lanes], 0.0)


def pick(rows, d, s):
    return [w[2 * d + s : 2 * d + s + 1] for w in rows]


def plane_rows(cell_ref, tables, s, lanes):
    first = cell_ref[0, s : s + 1, lanes] & (XB - 1)
    second = cell_ref[1, s : s + 1, lanes] & (YB - 1)
    return (
        placed_rows(first, [pick(t, 0, s) for t in tables], -8, XB + 8, False),
        placed_rows(second, [pick(t, 1, s) for t in tables], -8, YB + 8, False),
    )


def put(ph, pq, at, product):
    top, rest = split(product)
    ph[at : at + product.shape[0], :] = top
    pq[at : at + product.shape[0], :] = rest


ALL = pl.ds(0, ATOMS)


def give(total, s, pieces):
    for ref, at, count in pieces:
        for h in range(2):
            ref[2 * s + h] = total[at : at + count, h * 128 : h * 128 + 128]


def spread_rim_kernel(
    count_ref, cell_hbm, frac_hbm, charge_hbm, xr_ref, yr_ref, cr_ref,
    cell_ref, frac_ref, charge_ref, ph, pq, wh_ref, wl_ref, sems,
):
    copies = [
        pltpu.make_async_copy(source, target, sems.at[n])
        for n, (source, target) in enumerate(
            ((cell_hbm, cell_ref), (frac_hbm, frac_ref), (charge_hbm, charge_ref))
        )
    ]
    for copy in copies:
        copy.start()
    for copy in copies:
        copy.wait()
    levels, _ = atom_rows(frac_ref, ALL)
    for s in range(2):
        (first,), (second,) = plane_rows(cell_ref, [levels], s, ALL)
        place_tables(cell_ref[2, s : s + 1, :], [pick(levels, 2, s)], [(wh_ref.at[s], wl_ref.at[s])])
        second = second * live_charges(charge_ref, count_ref, s, 0, ALL)
        p, q = ph.at[s], pq.at[s]
        for x in range(RIM):
            put(p, q, x * YB, first[3 + x : 4 + x] * second[8:])
        for y in range(RIM):
            put(p, q, XRIM + y * XB, second[3 + y : 4 + y] * first[8:])
        corner = [second[3 + y : 4 + y] * first[:8] for y in range(RIM)]
        corner.append(jnp.zeros((8, ATOMS), F32))
        for y in range(0, RIM + 1, 2):
            put(p, q, XRIM + YRIM + y * 8, jnp.concatenate(corner[y : y + 2], axis=0))
        total = dot3((p[...], q[...]), (wh_ref[s], wl_ref[s]), ((1,), (1,)))
        give(total, s, ((xr_ref, 0, XRIM), (yr_ref, XRIM, YRIM), (cr_ref, XRIM + YRIM, CRIM)))


def spread_kernel(count_ref, cell_ref, frac_ref, charge_ref, mesh_ref, ph, pq, wh_ref, wl_ref):
    levels, _ = atom_rows(frac_ref, ALL)
    for s in range(2):
        (first,), (second,) = plane_rows(cell_ref, [levels], s, ALL)
        second = second * live_charges(charge_ref, count_ref, s, 0, ALL)
        place_tables(cell_ref[2, s : s + 1, :], [pick(levels, 2, s)], [(wh_ref.at[s], wl_ref.at[s])])
        p, q = ph.at[s], pq.at[s]
        for y in range(YB):
            put(p, q, y * XB, second[8 + y : 9 + y] * first[8:])
        total = dot3((p[...], q[...]), (wh_ref[s], wl_ref[s]), ((1,), (1,)))
        give(total, s, ((mesh_ref, 0, INNER),))


TALL, WIDE = XB + 8, YB + 8
SIDES = 2 * TALL + 2 * WIDE


def weight_kernel(count_ref, cell_ref, frac_ref, charge_ref, wh_ref, wl_ref, sh_ref, sl_ref, xy_ref):
    tables = atom_rows(frac_ref, ALL)
    for s in range(2):
        place_tables(
            cell_ref[2, s : s + 1, :],
            [pick(t, 2, s) for t in tables],
            [(wh_ref.at[s], wl_ref.at[s]), (sh_ref.at[s], sl_ref.at[s])],
        )
        xs, ys = plane_rows(cell_ref, tables, s, ALL)
        charges = -live_charges(charge_ref, count_ref, s, 0, ALL)
        xy_ref[s, :TALL, :] = xs[0]
        xy_ref[s, TALL : 2 * TALL, :] = xs[1]
        xy_ref[s, 2 * TALL : 2 * TALL + WIDE, :] = ys[0] * charges
        xy_ref[s, 2 * TALL + WIDE :, :] = ys[1] * charges


def side_weights(xy_ref, s, lanes):
    xy = xy_ref[s, :, lanes]
    return (
        (xy[:TALL], xy[TALL : 2 * TALL]),
        (xy[2 * TALL : 2 * TALL + WIDE], xy[2 * TALL + WIDE :]),
    )


def forward_z_kernel(mesh_ref, xr_ref, yr_ref, cr_ref, zc, out_ref, m):
    m[...] = mesh_ref[...]
    parts = []
    for s in range(2):
        base = (YB - RIM) * XB
        columns = []
        for h in range(2):
            k = 2 * s + h
            m[k, base : base + YRIM, :] += yr_ref[k]
            for x in range(RIM):
                rows = pl.ds(XB - RIM + x, YB, stride=XB)
                m[k, rows, :] += xr_ref[k, x * YB : x * YB + YB, :]
            for y in range(RIM):
                at = (YB - RIM + y) * XB + XB - 8
                m[k, at : at + 8, :] += cr_ref[k, y * 8 : y * 8 + 8]
            columns.append(m[k].T)
        parts.append(split(jnp.concatenate(columns, axis=0)))
    cosines, sines = (zc[0], zc[1]), (zc[2], zc[3])
    real = dot3(cosines, parts[0]) + dot3(sines, parts[1])
    imag = dot3(cosines, parts[1]) - dot3(sines, parts[0])
    for q, value in enumerate((real, imag)):
        for p in range(2):
            for b in range(4):
                out_ref[pl.ds(p * 8 + q * 4 + b, DEV, stride=16), :] = value[
                    p * DEV : (p + 1) * DEV, b * 128 : (b + 1) * 128
                ]


def exchange_blocks(pieces):
    lane = lax.broadcasted_iota(jnp.int32, pieces[0].shape, 1)
    for bit in (1, 2):
        upper = (lane // 32) & bit == bit
        fresh = list(pieces)
        for v in range(4):
            if v & bit == 0:
                a, b = pieces[v], pieces[v | bit]
                fresh[v] = jnp.where(upper, pltpu.roll(b, 32 * bit, 1), a)
                fresh[v | bit] = jnp.where(upper, b, pltpu.roll(a, 128 - 32 * bit, 1))
        pieces = fresh
    return pieces


def plane_kernel(buf_ref, green_ref, yc, xc, out_ref, d, o):
    cosines, sines = (xc[0], xc[1]), (xc[2], xc[3])
    planes = range(2)
    for p in planes:
        for c in range(COLS):
            for g in range(2):
                tiles = []
                for r in range(4):
                    at = ((g * 4 + r) * COLS + c) * 16 + p * 8
                    tiles.append(buf_ref[at : at + 8, :])
                for low, tile in enumerate(exchange_blocks(tiles)):
                    at = (c * 4 + low) * 8
                    d[p, at : at + 8, g * 128 : g * 128 + 128] = tile
    first = [dot3((yc[0], yc[1]), split(d[p])) for p in planes]
    parts = [(split(f[:K]), split(f[K:])) for f in first]
    parts = [
        (dot3(real, cosines) + dot3(imag, sines), dot3(imag, cosines) - dot3(real, sines))
        for real, imag in parts
    ]
    scaled = []
    for p in planes:
        green = jnp.concatenate(
            [green_ref[(r * 2 + p) * XB : (r * 2 + p + 1) * XB, :] for r in range(ROWS)], axis=0
        ) * (1.0 / float(K) ** 3)
        scaled.append([split(part * green) for part in parts[p]])
    parts = [
        (
            split(dot3(real, cosines) - dot3(imag, sines)),
            split(dot3(imag, cosines) + dot3(real, sines)),
        )
        for real, imag in scaled
    ]
    for p in planes:
        both = tuple(jnp.concatenate([a, b], axis=0) for a, b in zip(*parts[p]))
        o[p] = dot3((yc[2], yc[3]), both)
    for p in planes:
        for c in range(COLS):
            for g in range(2):
                tiles = []
                for low in range(4):
                    at = (c * 4 + low) * 8
                    tiles.append(o[p, at : at + 8, g * 128 : g * 128 + 128])
                for r, tile in enumerate(exchange_blocks(tiles)):
                    at = ((g * 4 + r) * COLS + c) * 16 + p * 8
                    out_ref[at : at + 8, :] = tile


def inverse_z_kernel(buf_ref, zc, fh_ref, fl_ref, xr_ref, yr_ref, cr_ref, m):
    cosines, sines = (zc[0], zc[1]), (zc[2], zc[3])
    parts = []
    for q in range(2):
        columns = []
        for p in range(2):
            blocks = []
            for b in range(4):
                blocks.append(buf_ref[pl.ds(p * 8 + q * 4 + b, DEV, stride=16), :].T)
            columns.append(jnp.concatenate(blocks, axis=0))
        parts.append(split(jnp.concatenate(columns, axis=1)))
    real, imag = parts
    fields = (
        dot3(real, cosines) - dot3(imag, sines),
        dot3(imag, cosines) + dot3(real, sines),
    )
    base = (YB - RIM) * XB
    for s in range(2):
        fh_ref[s], fl_ref[s] = split(fields[s])
        for h in range(2):
            k = 2 * s + h
            m[k] = fields[s][:, h * 128 : h * 128 + 128]
            yr_ref[k] = m[k, base : base + YRIM, :]
            for x in range(RIM):
                rows = pl.ds(XB - RIM + x, YB, stride=XB)
                xr_ref[k, x * YB : x * YB + YB, :] = m[k, rows, :]
            for y in range(RIM):
                at = (YB - RIM + y) * XB + XB - 8
                cr_ref[k, y * 8 : y * 8 + 8, :] = m[k, at : at + 8, :]


def row(pair, n):
    return pair[0][n : n + 1], pair[1][n : n + 1]


def weighed(plain, sloped, at, along, across):
    value, slope = across
    size = value.shape[0]
    sums = [None] * 3
    for n, (mine, mine_slope) in enumerate(along):
        rows = slice(at + n * size, at + (n + 1) * size)
        terms = (mine * plain[rows], mine_slope * plain[rows], mine * sloped[rows])
        sums = [term if n == 0 else old + term for old, term in zip(sums, terms)]
    return tuple(
        jnp.sum(total * side, axis=0, keepdims=True)
        for total, side in zip(sums, (slope, value, value))
    )


def chunks(body):
    def step(i, carry):
        at = pl.multiple_of(i * CHUNK, CHUNK)
        body(at, pl.ds(at, CHUNK))
        return carry

    lax.fori_loop(0, ATOMS // CHUNK, step, 0, unroll=2)


def gather_kernel(xy_ref, wh_ref, wl_ref, sh_ref, sl_ref, fh_ref, fl_ref, out_ref):
    def body(at, lanes):
        for s in range(2):
            xs, ys = side_weights(xy_ref, s, lanes)
            field = fh_ref[s], fl_ref[s]
            plain = dot3(field, (wh_ref[s, :, lanes], wl_ref[s, :, lanes]))
            sloped = dot3(field, (sh_ref[s, :, lanes], sl_ref[s, :, lanes]))
            lines = [row(ys, 8 + y) for y in range(YB)]
            forces = weighed(plain, sloped, 0, lines, (xs[0][8:], xs[1][8:]))
            for d in range(3):
                out_ref[d, s : s + 1, lanes] = forces[d]

    chunks(body)


def gather_rim_kernel(
    xy_ref, wh_ref, wl_ref, sh_ref, sl_ref, xr_ref, yr_ref, cr_ref, inner_ref, out_ref, fh, fl,
):
    for s in range(2):
        for h in range(2):
            k, columns = 2 * s + h, slice(h * 128, h * 128 + 128)
            corner = jnp.concatenate([cr_ref[k], jnp.zeros((8, 128), F32)], axis=0)
            for value, at in ((xr_ref[k], 0), (yr_ref[k], XRIM), (corner, XRIM + YRIM)):
                top, rest = split(value)
                fh[s, at : at + value.shape[0], columns] = top
                fl[s, at : at + value.shape[0], columns] = rest

    def body(at, lanes):
        for s in range(2):
            xs, ys = side_weights(xy_ref, s, lanes)
            field = fh[s], fl[s]
            plain = dot3(field, (wh_ref[s, :, lanes], wl_ref[s, :, lanes]))
            sloped = dot3(field, (sh_ref[s, :, lanes], sl_ref[s, :, lanes]))
            lines = [row(ys, 3 + y) for y in range(RIM)]
            columns = [row(xs, 3 + x) for x in range(RIM)]
            side = weighed(plain, sloped, 0, columns, (ys[0][8:], ys[1][8:]))
            edge = weighed(plain, sloped, XRIM, lines, (xs[0][8:], xs[1][8:]))
            corner = weighed(plain, sloped, XRIM + YRIM, lines, (xs[0][:8], xs[1][:8]))
            for d, e in ((0, 1), (1, 0), (2, 2)):
                force = inner_ref[d, s : s + 1, lanes] + side[e] + edge[d] + corner[d]
                out_ref[d, s : s + 1, lanes] = force

    chunks(body)


def green_kernel(in_ref, out_ref, m):
    for h in range(2):
        lanes = slice(h * 128, h * 128 + 128)
        m[...] = in_ref[:, lanes]
        for k in range(COLS):
            out_ref[k * XB : (k + 1) * XB, lanes] = m[pl.ds(k, XB, stride=COLS), :]


def call(kernel, flops, out_shape, operands, smem=(), hbm=(), scratch=(), limit=24):
    def spec(n):
        if n in hbm:
            return HBM_ALL
        return SMEM_ALL if n in smem else VMEM_ALL

    single = not isinstance(out_shape, list)
    shapes = [out_shape] if single else out_shape
    size = sum(math.prod(v.shape) * v.dtype.itemsize for v in list(operands) + shapes)
    return pl.pallas_call(
        kernel,
        out_shape=out_shape,
        in_specs=[spec(n) for n in range(len(operands))],
        out_specs=VMEM_ALL if single else [VMEM_ALL] * len(shapes),
        scratch_shapes=list(scratch),
        compiler_params=pltpu.CompilerParams(vmem_limit_bytes=limit * 2**20),
        cost_estimate=pl.CostEstimate(flops=int(flops), bytes_accessed=size, transcendentals=0),
    )(*operands)


def shape(*dims, dtype=F32):
    return jax.ShapeDtypeStruct(dims, dtype)


def shift(value, rows, cols):
    pairs = []
    for r in range(ROWS):
        for c in range(COLS):
            pairs.append((r * COLS + c, ((r + rows) % ROWS) * COLS + (c + cols) % COLS))
    return lax.ppermute(value, ("row", "col"), pairs)


def rims_moved(xr, yr, cr, by):
    yr = shift(yr, 0, by)
    xr = shift(xr, by, 0)
    cr = shift(cr, by, by)
    return xr, yr, cr


def everywhere(value):
    return lax.all_to_all(value, ("row", "col"), split_axis=0, concat_axis=0, tiled=True)


def shards(cell_index, fraction, charge, atom_count, influence):
    zc = jnp.asarray(z_tables())
    xc = jnp.asarray(x_tables())
    table = y_table()
    yc = jnp.asarray(np.stack(halves(table) + halves(np.ascontiguousarray(table.T))))

    cells = jnp.transpose(cell_index, (1, 0, 2))
    fractions = jnp.transpose(fraction, (1, 0, 2))
    counts = jnp.transpose(atom_count, (1, 0))
    atoms = (counts, cells, fractions, charge)
    rim_shapes = [shape(4, XRIM, 128), shape(4, YRIM, 128), shape(4, CRIM, 128)]
    weights = shape(2, K, ATOMS, dtype=BF16)

    table = pltpu.VMEM((2, K, ATOMS), BF16)
    xr, yr, cr = call(
        spread_rim_kernel, 6e9, rim_shapes, atoms,
        smem=(0,), hbm=(1, 2, 3), limit=60,
        scratch=[
            pltpu.VMEM((3, 2, ATOMS), jnp.int32),
            pltpu.VMEM((3, 2, ATOMS), F32),
            pltpu.VMEM((2, ATOMS), F32),
            pltpu.VMEM((2, RIMS + 8, ATOMS), BF16),
            pltpu.VMEM((2, RIMS + 8, ATOMS), BF16),
            table,
            table,
            pltpu.SemaphoreType.DMA((3,)),
        ],
    )
    later, _ = lax.optimization_barrier((influence, cr))
    xr, yr, cr = rims_moved(xr, yr, cr, -1)
    green = call(
        green_kernel, 1e8, shape(512, K), (later.reshape(XB * COLS, K),),
        scratch=[pltpu.VMEM((512, 128), F32)],
    )
    green = lax.all_to_all(
        green.reshape(ROWS, 64, K), "row", split_axis=0, concat_axis=0, tiled=True
    ).reshape(512, K)
    mesh = call(
        spread_kernel, 8e9, shape(4, INNER, 128), atoms,
        smem=(0,), limit=32,
        scratch=[pltpu.VMEM((2, INNER, ATOMS), BF16)] * 2 + [table] * 2,
    )
    packed = call(
        forward_z_kernel, 3e9, shape(DEV * 16, 128), (mesh, xr, yr, cr, zc),
        scratch=[pltpu.VMEM((4, INNER, 128), F32)],
    )
    packed = everywhere(packed.reshape(DEV, 16, 128)).reshape(DEV * 16, 128)
    wh, wl, gh, gl, xy = call(
        weight_kernel, 1e10, [weights] * 4 + [shape(2, SIDES, ATOMS)], atoms, smem=(0,),
        limit=60,
    )
    packed = call(
        plane_kernel, 6e9, shape(DEV * 16, 128), (packed, green, yc, xc),
        scratch=[pltpu.VMEM((2, 512, K), F32)] * 2,
    )
    packed = everywhere(packed.reshape(DEV, 16, 128)).reshape(DEV * 16, 128)
    fh, fl, xr, yr, cr = call(
        inverse_z_kernel, 3e9, [shape(2, INNER, K, dtype=BF16)] * 2 + rim_shapes,
        (packed, zc),
        scratch=[pltpu.VMEM((4, INNER, 128), F32)],
    )
    xr, yr, cr = rims_moved(xr, yr, cr, 1)
    inner = call(
        gather_kernel, 1.2e10, shape(3, 2, ATOMS),
        (xy, wh, wl, gh, gl, fh, fl),
    )
    forces = call(
        gather_rim_kernel, 8e9, shape(3, 2, ATOMS),
        (xy, wh, wl, gh, gl, xr, yr, cr, inner),
        scratch=[pltpu.VMEM((2, RIMS + 8, K), BF16)] * 2,
    )
    return jnp.transpose(forces, (1, 0, 2))


def solution(mesh):
    placed = (
        P(None, None, ("row", "col")),
        P(None, None, ("row", "col")),
        P(None, ("row", "col")),
        P(None, ("row", "col")),
        P("row", "col", None),
    )
    return jax.shard_map(
        shards, mesh=mesh, in_specs=placed, out_specs=P(None, None, ("row", "col")), check_vma=False
    )
```
